16 devices in a mesh: dp: 2 (over y, z), tp: 8 (over x, core).
Axes of the slice: x: 4, y: 2, z: 1, core: 2. Of those that a mesh axis runs over, the one named last changes fastest.
The devices are a block of a 4x4x8 slice.
Arguments:
- k_local: bfloat16 [6, 1024, 16, 256], P('dp', 'tp'), parts along dimension 0
- v_local: bfloat16 [6, 1024, 16, 256], P('dp', 'tp'), parts along dimension 0
- k_global: bfloat16 [6, 1024, 16, 256], P('dp', 'tp'), parts along dimension 0
- v_global: bfloat16 [6, 1024, 16, 256], P('dp', 'tp'), parts along dimension 0
- x_token: bfloat16 [6, 3072], P('dp'), parts along dimension 0
- w_q: bfloat16 [2, 3072, 4096], P(None, None, 'tp')
- w_k: bfloat16 [2, 3072, 4096], P(None, None, 'tp')
- w_v: bfloat16 [2, 3072, 4096], P(None, None, 'tp')
- w_o: bfloat16 [2, 4096, 3072], P(None, 'tp')
- w_gate: bfloat16 [2, 3072, 24576], P(None, None, 'tp')
- w_up: bfloat16 [2, 3072, 24576], P(None, None, 'tp')
- w_down: bfloat16 [2, 24576, 3072], P(None, 'tp')
- norm_gain: float32 [2, 4, 3072], replicated
- qk_gain: float32 [2, 2, 256], replicated
Outputs:
- output 1: bfloat16 [6, 3072], P('dp'), parts along dimension 0
- output 2: bfloat16 [6, 1024, 16, 256], P('dp', None, 'tp'), parts along dimension 0
- output 3: bfloat16 [6, 1024, 16, 256], P('dp', None, 'tp'), parts along dimension 0
- output 4: bfloat16 [6, 1152, 16, 256], P('dp', None, 'tp'), parts along dimension 0
- output 5: bfloat16 [6, 1152, 16, 256], P('dp', None, 'tp'), parts along dimension 0
There are 2 independent parts. The reference program is written for one: setup_inputs(seed, part) draws one part's arguments, and reference() takes and returns one part's arrays. A program takes and returns all parts, laid end to end along the dimension named above; an argument that names none is the same for every part.
All inputs are finite; a program needn't handle non-finite values.
Results may differ from the reference program's by a relative error of at most 0.0149703.
Values are sent between devices in bfloat16 or wider.
A program may use at most 768 MiB of HBM per device.

```python
import jax
import jax.numpy as jnp
from jax import lax

D = 3072
HEADS = 16
KV_HEADS = 16
HEAD = 256
FF = 24576
BATCH = 3
SEQ = 1024
WINDOW = 1024
NEW_SLOTS = 128
NORM_EPS = 1e-6
LOCAL_BASE = 10000.0
GLOBAL_BASE = 1000000.0
POS_SCALE = 8.0


def setup_inputs(seed: int = 0, part: int = 0) -> dict:
    part_key = jax.random.fold_in(jax.random.key(seed), part)
    cache_keys = jax.random.split(part_key, 5)
    weight_keys = jax.random.split(jax.random.key(seed + 1), 9)
    kv_shape = (BATCH, SEQ, KV_HEADS, HEAD)
    q_width = HEADS * HEAD
    kv_width = KV_HEADS * HEAD

    def normal_bf16(key_in, shape, scale):
        return (scale * jax.random.normal(key_in, shape, jnp.float32)).astype(jnp.bfloat16)

    return {
        "k_local": normal_bf16(cache_keys[0], kv_shape, 0.5),
        "v_local": normal_bf16(cache_keys[1], kv_shape, 1.0),
        "k_global": normal_bf16(cache_keys[2], kv_shape, 0.5),
        "v_global": normal_bf16(cache_keys[3], kv_shape, 1.0),
        "x_token": normal_bf16(cache_keys[4], (BATCH, D), 1.0),
        "w_q": normal_bf16(weight_keys[0], (2, D, q_width), D ** -0.5),
        "w_k": normal_bf16(weight_keys[1], (2, D, kv_width), D ** -0.5),
        "w_v": normal_bf16(weight_keys[2], (2, D, kv_width), 2.0 * D ** -0.5),
        "w_o": normal_bf16(weight_keys[3], (2, q_width, D), q_width ** -0.5),
        "w_gate": normal_bf16(weight_keys[4], (2, D, FF), D ** -0.5),
        "w_up": normal_bf16(weight_keys[5], (2, D, FF), D ** -0.5),
        "w_down": normal_bf16(weight_keys[6], (2, FF, D), FF ** -0.5),
        "norm_gain": 0.4 * jax.random.normal(weight_keys[7], (2, 4, D), jnp.float32),
        "qk_gain": 0.5 + 0.4 * jax.random.normal(weight_keys[8], (2, 2, HEAD), jnp.float32),
    }


def rms_norm(values, gain_vec):
    mean_sq = jnp.mean(values * values, axis=-1, keepdims=True)
    return values * lax.rsqrt(mean_sq + NORM_EPS) * (1.0 + gain_vec)


def rope_rotate(values, position, rope_base):
    half_dim = HEAD // 2
    inv_freq = rope_base ** (-2.0 * jnp.arange(half_dim, dtype=jnp.float32) / HEAD)
    angles = position * inv_freq
    cos_part = jnp.cos(angles)
    sin_part = jnp.sin(angles)
    first_half = values[..., :half_dim]
    second_half = values[..., half_dim:]
    return jnp.concatenate([first_half * cos_part - second_half * sin_part, second_half * cos_part + first_half * sin_part], axis=-1)


def project_qkv(hidden, layer_idx, w_q, w_k, w_v, norm_gain, qk_gain, position, rope_base):
    normed = rms_norm(hidden, norm_gain[layer_idx, 0]).astype(jnp.bfloat16)
    q_proj = jnp.dot(normed, w_q[layer_idx], preferred_element_type=jnp.float32).reshape(BATCH, HEADS, HEAD)
    k_proj = jnp.dot(normed, w_k[layer_idx], preferred_element_type=jnp.float32).reshape(BATCH, KV_HEADS, HEAD)
    v_proj = jnp.dot(normed, w_v[layer_idx], preferred_element_type=jnp.float32).reshape(BATCH, KV_HEADS, HEAD)
    q_new = rope_rotate(rms_norm(q_proj, qk_gain[layer_idx, 0]), position, rope_base).astype(jnp.bfloat16)
    k_new = rope_rotate(rms_norm(k_proj, qk_gain[layer_idx, 1]), position, rope_base).astype(jnp.bfloat16)
    return q_new, k_new, v_proj.astype(jnp.bfloat16)


def attend(q_new, k_cache, v_cache):
    group_size = HEADS // KV_HEADS

    def one_row(row_data):
        q_row, k_row, v_row = row_data
        q_grouped = q_row.reshape(KV_HEADS, group_size, HEAD).astype(jnp.float32)
        scores = jnp.einsum("kgd,tkd->kgt", q_grouped, k_row.astype(jnp.float32)) * HEAD ** -0.5
        attn_prob = jax.nn.softmax(scores, axis=-1).astype(jnp.bfloat16)
        weighted = jnp.einsum("kgt,tkd->kgd", attn_prob.astype(jnp.float32), v_row.astype(jnp.float32))
        return weighted.reshape(HEADS * HEAD).astype(jnp.bfloat16)

    return lax.map(one_row, (q_new, k_cache, v_cache))


def finish_layer(hidden, layer_idx, attn_out, w_o, w_gate, w_up, w_down, norm_gain):
    attn_proj = jnp.dot(attn_out, w_o[layer_idx], preferred_element_type=jnp.float32)
    hidden = hidden + rms_norm(attn_proj, norm_gain[layer_idx, 1])
    normed = rms_norm(hidden, norm_gain[layer_idx, 2]).astype(jnp.bfloat16)
    gate_proj = jnp.dot(normed, w_gate[layer_idx], preferred_element_type=jnp.float32)
    up_proj = jnp.dot(normed, w_up[layer_idx], preferred_element_type=jnp.float32)
    gated_act = (jax.nn.gelu(gate_proj, approximate=True) * up_proj).astype(jnp.bfloat16)
    down_proj = jnp.dot(gated_act, w_down[layer_idx], preferred_element_type=jnp.float32)
    return hidden + rms_norm(down_proj, norm_gain[layer_idx, 3])


def reference(k_local, v_local, k_global, v_global, x_token, w_q, w_k, w_v, w_o, w_gate, w_up, w_down, norm_gain, qk_gain):
    slot_shift = SEQ % WINDOW
    hidden = x_token.astype(jnp.float32)
    q_new, k_new, v_new = project_qkv(hidden, 0, w_q, w_k, w_v, norm_gain, qk_gain, float(SEQ), LOCAL_BASE)
    k_circular = jnp.roll(k_local[:, SEQ - WINDOW:], slot_shift, axis=1).at[:, slot_shift].set(k_new)
    v_circular = jnp.roll(v_local[:, SEQ - WINDOW:], slot_shift, axis=1).at[:, slot_shift].set(v_new)
    attn_out = attend(q_new, k_circular, v_circular)
    hidden = finish_layer(hidden, 0, attn_out, w_o, w_gate, w_up, w_down, norm_gain)
    hidden = hidden.astype(jnp.bfloat16).astype(jnp.float32)
    q_new, k_new, v_new = project_qkv(hidden, 1, w_q, w_k, w_v, norm_gain, qk_gain, SEQ / POS_SCALE, GLOBAL_BASE)
    zero_slots = jnp.zeros((BATCH, NEW_SLOTS - 1, KV_HEADS, HEAD), jnp.bfloat16)
    k_cache = jnp.concatenate([k_global, k_new[:, None], zero_slots], axis=1)
    v_cache = jnp.concatenate([v_global, v_new[:, None], zero_slots], axis=1)
    attn_out = attend(q_new, k_cache[:, :SEQ + 1], v_cache[:, :SEQ + 1])
    hidden = finish_layer(hidden, 1, attn_out, w_o, w_gate, w_up, w_down, norm_gain)
    return hidden.astype(jnp.bfloat16), k_circular, v_circular, k_cache, v_cache
```

```python
import functools

import jax
import jax.numpy as jnp
import numpy as np
from jax import lax
from jax.experimental import pallas as pl
from jax.experimental.pallas import tpu as pltpu
from jax.sharding import PartitionSpec as P

WINDOW = 1024
NEW_SLOTS = 128
NORM_EPS = 1e-6
ROPE_BASES = (10000.0, 1000000.0)
POS_SCALES = (1.0, 8.0)
NEG = -3.0e38
MESH = pl.DeviceIdType.MESH
LANES = 128
ROWS = 8
RING = 8
CHUNK = 512
HALVES = 2
FIRST_UNITS = 2
ROUND_UNITS = (1, 1, 1, 1, 3, 1, 1)
ROUNDS = len(ROUND_UNITS)


def rms_norm(values, gain_vec):
    mean_sq = jnp.mean(values * values, axis=-1, keepdims=True)
    return values * lax.rsqrt(mean_sq + NORM_EPS) * (1.0 + gain_vec)


def kernel(cfg, *refs):
    groups, layers, batch, seq_dev, heads, head_dim, width, ff_dev = cfg
    n_in, n_out = 2 * len(range(4)) + 11, 5
    ins, outs, scr = refs[:n_in], refs[n_in:n_in + n_out], refs[n_in + n_out:]
    views, caches = ins[:4], ins[4:8]
    x_hbm, wq, wk, wv, wo, wg, wu, wd, ng_hbm, qk_hbm, rope_hbm = ins[8:]
    cache_out, h_out = outs[:4], outs[4]
    (ring, wo_buf, kv, x_vm, ng, qkg, rope, h_ref, lhs, acc, q_all, st_all, o_all, part, rs_all, ag_all,
     ring_sem, wo_sem, kv_sem, small_sem, self_sem, bulk_send, bulk_recv, r_send, r_recv) = scr
    me = lax.axis_index("tp")
    per_tile = heads // 2
    pairs = per_tile // 2
    seq = seq_dev * groups
    half_dim = head_dim // 2
    ff_items = ff_dev // CHUNK
    wd_items = width // CHUNK
    per_layer = 3 + 2 * ff_items + wd_items
    items = layers * per_layer

    def issue(item):
        item = jnp.asarray(item, jnp.int32)
        layer = item // per_layer
        r = item % per_layer
        slot = item % RING
        dst = ring.at[slot]
        sem = ring_sem.at[slot]
        for pos, ref in enumerate((wq, wk, wv)):
            @pl.when(r == pos)
            def _(ref=ref):
                pltpu.make_async_copy(ref.at[layer], dst, sem).start()
        for par, ref in enumerate((wg, wu)):
            @pl.when((r >= 3) & (r < 3 + 2 * ff_items) & ((r - 3) % 2 == par))
            def _(ref=ref):
                col = pl.multiple_of(jnp.clip((r - 3) // 2, 0, ff_items - 1) * CHUNK, CHUNK)
                pltpu.make_async_copy(ref.at[layer, :, pl.ds(col, CHUNK)], dst, sem).start()

        @pl.when(r >= 3 + 2 * ff_items)
        def _():
            col = pl.multiple_of(jnp.clip(r - 3 - 2 * ff_items, 0, wd_items - 1) * CHUNK, CHUNK)
            pltpu.make_async_copy(wd.at[layer, :, pl.ds(col, CHUNK)], dst, sem).start()

    def stream(first, count):
        def step(t, carry):
            item = first + t
            slot = item % RING
            pltpu.make_async_copy(wq.at[0], ring.at[slot], ring_sem.at[slot]).wait()
            acc[t] = jnp.dot(lhs[...], ring[slot], preferred_element_type=jnp.float32)

            @pl.when(item + RING < items)
            def _():
                issue(item + RING)
            return carry
        lax.fori_loop(0, count, step, 0)

    small = [pltpu.make_async_copy(s, d, small_sem.at[n]) for n, (s, d) in enumerate(
        ((x_hbm, x_vm), (ng_hbm, ng), (qk_hbm, qkg), (rope_hbm, rope)))]
    for c in small:
        c.start()
    for n in range(3):
        issue(n)
    kv_copies = [pltpu.make_async_copy(caches[n], kv.at[n], kv_sem.at[n]) for n in range(4)]
    wo_copies = [pltpu.make_async_copy(wo.at[n], wo_buf, wo_sem.at[n]) for n in range(layers)]
    kv_copies[0].start()
    kv_copies[1].start()
    wo_copies[0].start()
    for n in range(3, RING):
        issue(n)

    barrier = pltpu.get_barrier_semaphore()
    for k in range(1, groups):
        pl.semaphore_signal(barrier, inc=1, device_id={"tp": (me + k) % groups}, device_id_type=MESH)
    pl.semaphore_wait(barrier, groups - 1)

    span = seq_dev // HALVES
    units = [(c, b, f) for c in range(4) for b in range(batch) for f in range(HALVES)]
    chips = groups // 2
    order = [(dx, dc) for dc in range(2) for dx in (1, chips - 1, *range(2, chips - 1))] + [(0, 1)]
    chip, core = me // 2, me % 2

    def peer(dx, dc):
        return ((chip + dx) % chips) * 2 + (core + dc) % 2

    def view_of(c, owner, b, start, size):
        return views[c].at[b, pl.ds(start, size), owner // pairs, :, owner % pairs]

    queue = list(units)

    def bulk(count):
        for _ in range(min(count, len(queue))):
            c, b, f = queue.pop(0)
            for k, (dx, dc) in enumerate(order):
                dst = peer(dx, dc)
                pltpu.make_async_remote_copy(
                    view_of(c, dst, b, f * span, span),
                    cache_out[c].at[b, pl.ds(me * seq_dev + f * span, span)],
                    bulk_send.at[c, k], bulk_recv.at[c, k],
                    device_id={"tp": dst}, device_id_type=MESH).start()

    bulk(FIRST_UNITS)
    self_copies = [pltpu.make_async_copy(
        view_of(c, me, b, 0, seq_dev), cache_out[c].at[b, pl.ds(me * seq_dev, seq_dev)], self_sem.at[c, b])
        for c in range(4) for b in range(batch)]
    for c in self_copies:
        c.start()
    kv_copies[2].start()
    kv_copies[3].start()

    sent = []

    def send(rnd, src_of, dst_ref):
        got = []
        for k in range(1, groups):
            d = (me + k) % groups
            c = pltpu.make_async_remote_copy(src_of(d), dst_ref.at[me], r_send.at[rnd, k], r_recv.at[rnd, k],
                                             device_id={"tp": d}, device_id_type=MESH)
            c.start()
            got.append(c)
        sent.extend(got)
        return got

    row = lax.broadcasted_iota(jnp.int32, (ROWS, LANES), 0)
    lane = lax.broadcasted_iota(jnp.int32, (ROWS, LANES), 1)
    even = lax.broadcasted_iota(jnp.int32, (ROWS, 1), 0) % 2 == 0
    lane_head = lane % heads
    own = (lane_head == 2 * me + row % 2) & (row < 2 * batch)
    col_tiles = seq_dev * heads // LANES
    row64 = lax.broadcasted_iota(jnp.int32, (groups * ROWS, LANES), 0)
    lane64 = lax.broadcasted_iota(jnp.int32, (groups * ROWS, LANES), 1)
    head_hit = (lane64 % heads) == 2 * (row64 // ROWS) + row64 % 2
    hits = [jnp.tile(head_hit & ((row64 % ROWS) // 2 == b), (1, col_tiles)) for b in range(batch)]
    wide_row = lax.broadcasted_iota(jnp.int32, (ROWS, seq_dev * heads), 0)
    wide_col = lax.broadcasted_iota(jnp.int32, (ROWS, seq_dev * heads), 1)
    paired = (wide_col % 2 == wide_row % 2) & (wide_row < 2 * batch)

    def fold(x, op):
        out = x[:, :LANES]
        for n in range(1, x.shape[1] // LANES):
            out = op(out, x[:, n * LANES:(n + 1) * LANES])
        shift = heads
        while shift < LANES:
            out = op(out, pltpu.roll(out, shift, 1))
            shift *= 2
        return out

    def rope_rotate(x, layer):
        cos, sin = rope[layer, 0:1, :], rope[layer, 1:2, :]
        a, b = x[:, :half_dim], x[:, half_dim:]
        return jnp.concatenate([a * cos - b * sin, b * cos + a * sin], axis=-1)

    def pick(y):
        return jnp.where(even, y[:, :head_dim], y[:, head_dim:])

    def all_reduce(rnd, layer, slot):
        got = send(rnd, lambda d: part.at[slot, d], rs_all.at[slot])
        bulk(ROUND_UNITS[(rnd % ROUNDS)])
        rs_all[slot, me] = part[slot, me]
        for c in got:
            c.wait_recv()
        total = rs_all[slot, 0]
        for s in range(1, groups):
            total = total + rs_all[slot, s]
        ag_all[slot, me] = total
        got = send(rnd + 1, lambda d: ag_all.at[slot, me], ag_all.at[slot])
        bulk(ROUND_UNITS[(rnd + 1) % ROUNDS])
        for c in got:
            c.wait_recv()
        return jnp.concatenate([ag_all[slot, s] for s in range(groups)], axis=-1)

    for c in small:
        c.wait()
    x = x_vm[...].astype(jnp.float32)
    wide8 = lax.broadcasted_iota(jnp.int32, (ROWS, width), 0) // 2
    h0 = jnp.zeros((ROWS, width), jnp.float32)
    for b in range(batch):
        h0 = jnp.where(wide8 == b, jnp.broadcast_to(x[b:b + 1], (ROWS, width)), h0)
    h_ref[...] = h0

    new_rows = []
    for layer in range(layers):
        rnd = layer * ROUNDS
        base = layer * per_layer
        lhs[...] = rms_norm(h_ref[...], ng[layer, 0:1, :]).astype(jnp.bfloat16)
        stream(base, 3)
        q = rope_rotate(rms_norm(pick(acc[0]), qkg[layer, 0:1, :]), layer).astype(jnp.bfloat16).astype(jnp.float32)
        q_all[layer, me] = q
        got = send(rnd, lambda d: q_all.at[layer, me], q_all.at[layer])
        bulk(ROUND_UNITS[0])
        k_new = rope_rotate(rms_norm(pick(acc[1]), qkg[layer, 1:2, :]), layer).astype(jnp.bfloat16).astype(jnp.float32)
        v_new = pick(acc[2]).astype(jnp.bfloat16).astype(jnp.float32)
        new_rows.append((k_new, v_new))
        scale = head_dim ** -0.5
        s_new = jnp.sum(q * k_new, axis=-1, keepdims=True) * scale
        kv_copies[2 * layer].wait()
        kv_copies[2 * layer + 1].wait()
        for c in got:
            c.wait_recv()
        q64 = q_all[layer].reshape(groups * ROWS, head_dim).astype(jnp.bfloat16)
        scores = jnp.zeros((ROWS, seq_dev * heads), jnp.float32)
        for b in range(batch):
            s = lax.dot_general(q64, kv[2 * layer, b], (((1,), (1,)), ((), ())), preferred_element_type=jnp.float32)
            s = jnp.where(hits[b], s, 0.0)
            for d in range(groups):
                scores = scores + s[d * ROWS:(d + 1) * ROWS]
        valid = paired
        if layer == 0:
            valid = valid & (me * seq_dev + wide_col // heads >= seq + 1 - WINDOW)
        scores = jnp.where(valid, scores * scale, NEG)
        m_loc = fold(scores, jnp.maximum)
        m_loc = jnp.where(own, jnp.maximum(m_loc, s_new), m_loc)
        ex = jnp.where(valid, jnp.exp(scores - jnp.tile(m_loc, (1, col_tiles))), 0.0)
        l_loc = fold(ex, jnp.add)
        l_loc = jnp.where(own, l_loc + jnp.exp(s_new - m_loc), l_loc)
        st_all[layer, me] = jnp.where(lane < LANES // 2, m_loc, l_loc)
        got = send(rnd + 1, lambda d: st_all.at[layer, me], st_all.at[layer])
        bulk(ROUND_UNITS[1])
        for c in got:
            c.wait_recv()
        stats = [st_all[layer, s] for s in range(groups)]
        low = lane < LANES // 2
        ms = [jnp.where(low, t, pltpu.roll(t, LANES // 2, 1)) for t in stats]
        ls = [jnp.where(low, pltpu.roll(t, LANES // 2, 1), t) for t in stats]
        m_all = functools.reduce(jnp.maximum, ms)
        l_all = functools.reduce(jnp.add, [l * jnp.exp(m - m_all) for m, l in zip(ms, ls)])
        l_all = jnp.where(row < 2 * batch, jnp.maximum(l_all, 1e-30), 1.0)
        prob = jnp.where(valid, jnp.exp(scores - jnp.tile(m_all, (1, col_tiles))) / jnp.tile(l_all, (1, col_tiles)), 0.0)
        p_new = jnp.where(own & (lane < heads), jnp.exp(jnp.minimum(s_new - m_all, 0.0)) / l_all, 0.0)
        p_new = jnp.sum(p_new, axis=-1, keepdims=True).astype(jnp.bfloat16).astype(jnp.float32)
        prob64 = jnp.concatenate([prob] * groups, axis=0)
        o_part = jnp.zeros((groups * ROWS, head_dim), jnp.float32)
        for b in range(batch):
            o_part = o_part + jnp.dot(jnp.where(hits[b], prob64, 0.0).astype(jnp.bfloat16), kv[2 * layer + 1, b],
                                      preferred_element_type=jnp.float32)
        o_all[layer, 0] = o_part.reshape(groups, ROWS, head_dim)
        got = send(rnd + 2, lambda d: o_all.at[layer, 0, d], o_all.at[layer, 1])
        bulk(ROUND_UNITS[2])
        o_all[layer, 1, me] = o_all[layer, 0, me]
        for c in got:
            c.wait_recv()
        o = p_new * v_new
        for s in range(groups):
            o = o + o_all[layer, 1, s]
        o = o.astype(jnp.bfloat16).astype(jnp.float32)
        o = jnp.concatenate([jnp.where(even, o, 0.0), jnp.where(even, 0.0, o)], axis=-1).astype(jnp.bfloat16)
        wo_copies[layer].wait()
        piece = width // groups
        for d in range(groups):
            y = jnp.dot(o, wo_buf[:, d * piece:(d + 1) * piece], preferred_element_type=jnp.float32)
            part[2 * layer, d] = y + jnp.where(even, pltpu.roll(y, ROWS - 1, 0), pltpu.roll(y, 1, 0))
        if layer + 1 < layers:
            wo_copies[layer + 1].start()
        hidden = h_ref[...] + rms_norm(all_reduce(rnd + 3, layer, 2 * layer), ng[layer, 1:2, :])
        h_ref[...] = hidden
        lhs[...] = rms_norm(hidden, ng[layer, 2:3, :]).astype(jnp.bfloat16)
        stream(base + 3, 2 * ff_items)
        for n in range(ff_items):
            lhs[:, n * CHUNK:(n + 1) * CHUNK] = (
                jax.nn.gelu(acc[2 * n], approximate=True) * acc[2 * n + 1]).astype(jnp.bfloat16)
        stream(base + 3 + 2 * ff_items, wd_items)
        full = jnp.concatenate([acc[n] for n in range(wd_items)], axis=-1)
        for d in range(groups):
            part[2 * layer + 1, d] = full[:, d * piece:(d + 1) * piece]
        hidden = h_ref[...] + rms_norm(all_reduce(rnd + 5, layer, 2 * layer + 1), ng[layer, 3:4, :])
        h_ref[...] = hidden.astype(jnp.bfloat16).astype(jnp.float32)

    bulk(len(queue))
    for b in range(batch):
        h_out[b:b + 1, :] = h_ref[2 * b:2 * b + 1, :].astype(jnp.bfloat16)
    zeros = jnp.zeros((NEW_SLOTS - 1, 2, 2, LANES), jnp.bfloat16)
    for c in (2, 3):
        for b in range(batch):
            cache_out[c][b, seq + 1:] = zeros
    for c in sent:
        c.wait_send()
    for c in self_copies:
        c.wait()
    for c in range(4):
        for k, (dx, dc) in enumerate(order):
            src = peer(-dx % chips, dc)
            region = cache_out[c].at[0:batch, pl.ds(src * seq_dev, seq_dev)]
            whole = pltpu.make_async_remote_copy(region, region, bulk_send.at[c, k], bulk_recv.at[c, k],
                                                 device_id={"tp": peer(dx, dc)}, device_id_type=MESH)
            whole.wait_recv()
            whole.wait_send()
    slots = (seq % WINDOW, seq)
    for layer in range(layers):
        for n in range(2):
            for b in range(batch):
                for ct in range(2):
                    cache_out[2 * layer + n][b, slots[layer], ct] = new_rows[layer][n][
                        2 * b:2 * b + 2, ct * LANES:(ct + 1) * LANES].astype(jnp.bfloat16)


def solution(mesh):
    groups = mesh.shape["tp"]
    cache_in = P("dp", "tp", None, None)
    cache_out = P("dp", None, "tp", None)
    token_spec = P("dp", None)
    col_split = P(None, None, "tp")
    row_split = P(None, "tp", None)
    replicated = P()

    def per_device(k_local, v_local, k_global, v_global, x_token, w_q, w_k, w_v, w_o, w_gate, w_up, w_down, norm_gain, qk_gain):
        batch, seq_dev, heads, head_dim = k_local.shape
        layers, width, _ = w_q.shape
        ff_dev = w_gate.shape[2]
        seq = seq_dev * groups
        tiles, pairs, cols = heads // 8, 4, head_dim // LANES
        caches = (k_local, v_local, k_global, v_global)
        views = [c.reshape(batch, seq_dev, tiles, pairs, 2, cols, LANES).transpose(0, 1, 2, 5, 3, 4, 6) for c in caches]
        flat = [c.reshape(batch, seq_dev * heads, head_dim) for c in caches]
        inv_freq = [b ** (-2.0 * np.arange(head_dim // 2) / head_dim) for b in ROPE_BASES]
        angles = [seq / s * f for s, f in zip(POS_SCALES, inv_freq)]
        rope = jnp.asarray(np.stack([np.stack([np.cos(a), np.sin(a)]) for a in angles]), jnp.float32)
        any_spec = pl.BlockSpec(memory_space=pl.ANY)
        vmem_spec = pl.BlockSpec(memory_space=pltpu.VMEM)
        cfg = (groups, layers, batch, seq_dev, heads, head_dim, width, ff_dev)
        slots = (WINDOW, WINDOW, seq + NEW_SLOTS, seq + NEW_SLOTS)
        piece = width // groups
        rounds = layers * ROUNDS
        res = pl.pallas_call(
            functools.partial(kernel, cfg),
            in_specs=[any_spec] * 19,
            out_specs=[vmem_spec] * 5,
            out_shape=[pltpu.VMEM((batch, s, 2, 2, LANES), jnp.bfloat16) for s in slots]
            + [jax.ShapeDtypeStruct((batch, width), jnp.bfloat16)],
            scratch_shapes=[
                pltpu.VMEM((RING, width, CHUNK), jnp.bfloat16),
                pltpu.VMEM((w_o.shape[1], width), jnp.bfloat16),
                pltpu.VMEM((4, batch, seq_dev * heads, head_dim), jnp.bfloat16),
                pltpu.VMEM(x_token.shape, jnp.bfloat16),
                pltpu.VMEM(norm_gain.shape, jnp.float32),
                pltpu.VMEM(qk_gain.shape, jnp.float32),
                pltpu.VMEM(rope.shape, jnp.float32),
                pltpu.VMEM((ROWS, width), jnp.float32),
                pltpu.VMEM((ROWS, width), jnp.bfloat16),
                pltpu.VMEM((2 * ff_dev // CHUNK, ROWS, CHUNK), jnp.float32),
                pltpu.VMEM((layers, groups, ROWS, head_dim), jnp.float32),
                pltpu.VMEM((layers, groups, ROWS, LANES), jnp.float32),
                pltpu.VMEM((layers, 2, groups, ROWS, head_dim), jnp.float32),
                pltpu.VMEM((2 * layers, groups, ROWS, piece), jnp.float32),
                pltpu.VMEM((2 * layers, groups, ROWS, piece), jnp.float32),
                pltpu.VMEM((2 * layers, groups, ROWS, piece), jnp.float32),
                pltpu.SemaphoreType.DMA((RING,)),
                pltpu.SemaphoreType.DMA((layers,)),
                pltpu.SemaphoreType.DMA((4,)),
                pltpu.SemaphoreType.DMA((4,)),
                pltpu.SemaphoreType.DMA((4, batch)),
                pltpu.SemaphoreType.DMA((4, groups - 1)),
                pltpu.SemaphoreType.DMA((4, groups - 1)),
                pltpu.SemaphoreType.DMA((rounds, groups)),
                pltpu.SemaphoreType.DMA((rounds, groups)),
            ],
            compiler_params=pltpu.CompilerParams(
                collective_id=0, has_side_effects=True, vmem_limit_bytes=44 * 1024 * 1024),
        )(*views, *flat, x_token, w_q, w_k, w_v, w_o, w_gate, w_up, w_down, norm_gain, qk_gain, rope)
        outs = [y.transpose(0, 1, 3, 2, 4).reshape(batch, y.shape[1], 2, head_dim) for y in res[:4]]
        return (res[4], *outs)

    return jax.shard_map(per_device, mesh=mesh, in_specs=(cache_in, cache_in, cache_in, cache_in, token_spec, col_split, col_split, col_split, row_split, col_split, col_split, row_split, replicated, replicated), out_specs=(token_spec, cache_out, cache_out, cache_out, cache_out), check_vma=False)
```

```python
import functools

import jax
import jax.numpy as jnp
import numpy as np
from jax import lax
from jax.experimental import pallas as pl
from jax.experimental.pallas import tpu as pltpu
from jax.sharding import PartitionSpec as P

WINDOW = 1024
NEW_SLOTS = 128
NORM_EPS = 1e-6
ROPE_BASES = (10000.0, 1000000.0)
POS_SCALES = (1.0, 8.0)
NEG = -3.0e38
MESH = pl.DeviceIdType.MESH
LANES = 128
ROWS = 8
TOKENS = 4
RING = 8
CHUNK = 512
SPLITS = 4
FIRST_UNITS = 4
ROUND_UNITS = (2, 2, 2, 2, 6, 2, 2, 2, 2, 2, 2, 6, 2, 2)
ROUNDS = 7
STEPS = 9


def rms_norm(values, gain_vec):
    mean_sq = jnp.mean(values * values, axis=-1, keepdims=True)
    return values * lax.rsqrt(mean_sq + NORM_EPS) * (1.0 + gain_vec)


def kernel(cfg, *refs):
    groups, layers, batch, seq_dev, heads, head_dim, width, ff_dev = cfg
    n_in, n_out = 2 * len(range(4)) + 11, 5
    ins, outs, scr = refs[:n_in], refs[n_in:n_in + n_out], refs[n_in + n_out:]
    views, caches = ins[:4], ins[4:8]
    x_hbm, wq, wk, wv, wo, wg, wu, wd, ng_hbm, qk_hbm, rope_hbm = ins[8:]
    cache_out, h_out = outs[:4], outs[4]
    (ring, wo_buf, kv, x_vm, ng, qkg, rope, h_ref, lhs, acc, q_all, st_all, o_part, o_pair, o_sum, o_cross,
     part, rs_pair, rs_sum, rs_cross, ag_all,
     ring_sem, wo_sem, kv_sem, small_sem, self_sem, bulk_send, bulk_recv, r_send, r_recv) = scr
    me = lax.axis_index("tp")
    per_tile = heads // 2
    pairs = per_tile // 2
    seq = seq_dev * groups
    half_dim = head_dim // 2
    ff_items = ff_dev // CHUNK
    wd_items = width // CHUNK
    per_layer = 3 + 2 * ff_items + wd_items
    items = layers * per_layer

    def issue(item):
        item = jnp.asarray(item, jnp.int32)
        layer = item // per_layer
        r = item % per_layer
        slot = item % RING
        dst = ring.at[slot]
        sem = ring_sem.at[slot]
        for pos, ref in enumerate((wq, wk, wv)):
            @pl.when(r == pos)
            def _(ref=ref):
                pltpu.make_async_copy(ref.at[layer], dst, sem).start()
        for par, ref in enumerate((wg, wu)):
            @pl.when((r >= 3) & (r < 3 + 2 * ff_items) & ((r - 3) % 2 == par))
            def _(ref=ref):
                col = pl.multiple_of(jnp.clip((r - 3) // 2, 0, ff_items - 1) * CHUNK, CHUNK)
                pltpu.make_async_copy(ref.at[layer, :, pl.ds(col, CHUNK)], dst, sem).start()

        @pl.when(r >= 3 + 2 * ff_items)
        def _():
            col = pl.multiple_of(jnp.clip(r - 3 - 2 * ff_items, 0, wd_items - 1) * CHUNK, CHUNK)
            pltpu.make_async_copy(wd.at[layer, :, pl.ds(col, CHUNK)], dst, sem).start()

    def stream(first, count):
        def step(t, carry):
            item = first + t
            slot = item % RING
            pltpu.make_async_copy(wq.at[0], ring.at[slot], ring_sem.at[slot]).wait()
            acc[t] = jnp.dot(lhs[...], ring[slot], preferred_element_type=jnp.float32)

            @pl.when(item + RING < items)
            def _():
                issue(item + RING)
            return carry
        lax.fori_loop(0, count, step, 0)

    barrier = pltpu.get_barrier_semaphore()
    for k in range(1, groups):
        pl.semaphore_signal(barrier, inc=1, device_id={"tp": (me + k) % groups}, device_id_type=MESH)
    small = [pltpu.make_async_copy(s, d, small_sem.at[n]) for n, (s, d) in enumerate(
        ((x_hbm, x_vm), (ng_hbm, ng), (qk_hbm, qkg), (rope_hbm, rope)))]
    for c in small:
        c.start()
    for n in range(3):
        issue(n)
    kv_copies = [pltpu.make_async_copy(caches[n], kv.at[n], kv_sem.at[n]) for n in range(4)]
    wo_copies = [pltpu.make_async_copy(wo.at[n], wo_buf, wo_sem.at[n]) for n in range(layers)]
    kv_copies[0].start()
    kv_copies[1].start()
    wo_copies[0].start()
    for n in range(3, RING):
        issue(n)

    pl.semaphore_wait(barrier, groups - 1)

    span = seq_dev // SPLITS
    units = [(c, b, f) for c in range(4) for b in range(batch) for f in range(SPLITS)]
    chips = groups // 2
    order = [(dx, dc) for dc in range(2) for dx in (1, chips - 1, *range(2, chips - 1))] + [(0, 1)]
    chip, core = me // 2, me % 2

    def peer(dx, dc):
        return ((chip + dx) % chips) * 2 + (core + dc) % 2

    def view_of(c, owner, b, start, size):
        return views[c].at[b, pl.ds(start, size), owner // pairs, :, owner % pairs]

    queue = list(units)

    def bulk(count):
        for _ in range(min(count, len(queue))):
            c, b, f = queue.pop(0)
            for k, (dx, dc) in enumerate(order):
                dst = peer(dx, dc)
                pltpu.make_async_remote_copy(
                    view_of(c, dst, b, f * span, span),
                    cache_out[c].at[b, pl.ds(me * seq_dev + f * span, span)],
                    bulk_send.at[c], bulk_recv.at[c],
                    device_id={"tp": dst}, device_id_type=MESH).start()

    bulk(FIRST_UNITS)
    self_copies = [pltpu.make_async_copy(
        view_of(c, me, b, 0, seq_dev), cache_out[c].at[b, pl.ds(me * seq_dev, seq_dev)], self_sem.at[c])
        for c in range(4) for b in range(batch)]
    for c in self_copies:
        c.start()
    kv_copies[2].start()
    kv_copies[3].start()

    sibling = chip * 2 + 1 - core
    pending = {}

    def start_round(step, copies, size_of):
        finish_sends(step)
        for src, dst, device in copies:
            pltpu.make_async_remote_copy(src, dst, r_send.at[step], r_recv.at[step],
                                         device_id={"tp": device}, device_id_type=MESH).start()
        pending[step] = pltpu.make_async_remote_copy(size_of, size_of, r_send.at[step], r_recv.at[step],
                                                     device_id={"tp": sibling}, device_id_type=MESH)
        return pending[step]

    def finish_sends(step):
        if step in pending:
            pending.pop(step).wait_send()

    others = [(chip + dx) % chips for dx in (1, chips - 1, *range(2, chips - 1))]

    def gather_cross(step, ref, units):
        got = start_round(step, [(ref.at[core, chip], ref.at[core, chip], t * 2 + core) for t in others],
                          ref.at[core, pl.ds(0, chips - 1)])
        bulk(units)
        got.wait_recv()

    def gather_pair(step, ref):
        start_round(step, [(ref.at[core], ref.at[core], sibling)], ref.at[core]).wait_recv()

    def scatter(step, mine, pair, summed, cross, units):
        start_round(step, [(mine.at[1 - core], pair, sibling)], pair).wait_recv()
        for t in range(chips):
            summed[t] = mine[core, t] + pair[t]
        got = start_round(step + 1, [(summed.at[t], cross.at[chip], t * 2 + core) for t in others],
                          cross.at[pl.ds(0, chips - 1)])
        bulk(units)
        cross[chip] = summed[chip]
        got.wait_recv()
        total = cross[0]
        for t in range(1, chips):
            total = total + cross[t]
        return total

    row = lax.broadcasted_iota(jnp.int32, (ROWS, LANES), 0)
    lane = lax.broadcasted_iota(jnp.int32, (ROWS, LANES), 1)
    even = lax.broadcasted_iota(jnp.int32, (ROWS, 1), 0) % 2 == 0
    lane_head = lane % heads
    own = (lane_head == 2 * me + row % 2) & (row < 2 * batch)
    col_tiles = seq_dev * heads // LANES
    row64 = lax.broadcasted_iota(jnp.int32, (groups * ROWS, LANES), 0)
    lane64 = lax.broadcasted_iota(jnp.int32, (groups * ROWS, LANES), 1)
    head_hit = (lane64 % heads) == 2 * (row64 // ROWS) + row64 % 2
    hits = [jnp.tile(head_hit & ((row64 % ROWS) // 2 == b), (1, col_tiles)) for b in range(batch)]
    wide_row = lax.broadcasted_iota(jnp.int32, (ROWS, seq_dev * heads), 0)
    wide_col = lax.broadcasted_iota(jnp.int32, (ROWS, seq_dev * heads), 1)
    paired = (wide_col % 2 == wide_row % 2) & (wide_row < 2 * batch)

    def fold(x, op):
        out = x[:, :LANES]
        for n in range(1, x.shape[1] // LANES):
            out = op(out, x[:, n * LANES:(n + 1) * LANES])
        shift = heads
        while shift < LANES:
            out = op(out, pltpu.roll(out, shift, 1))
            shift *= 2
        return out

    def rope_rotate(x, layer):
        cos, sin = rope[layer, 0:1, :], rope[layer, 1:2, :]
        a, b = x[:, :half_dim], x[:, half_dim:]
        return jnp.concatenate([a * cos - b * sin, b * cos + a * sin], axis=-1)

    row1 = lax.broadcasted_iota(jnp.int32, (ROWS, 1), 0)

    def pick(y):
        y = jnp.where(row1 == 0, y, jnp.where(row1 < 3, pltpu.roll(y, 1, 0), jnp.where(
            row1 < 5, pltpu.roll(y, 2, 0), pltpu.roll(y, 3, 0))))
        return jnp.where(even, y[:, :head_dim], y[:, head_dim:])

    def merge(y):
        y = y + pltpu.roll(y, ROWS - 1, 0)
        return jnp.where(row1 == 0, y, jnp.where(row1 == 1, pltpu.roll(y, ROWS - 1, 0), jnp.where(
            row1 == 2, pltpu.roll(y, ROWS - 2, 0), 0.0)))

    def all_reduce(rnd, slot):
        ag_all[slot, core, chip] = scatter(5, part.at[slot], rs_pair.at[slot], rs_sum.at[slot], rs_cross.at[slot],
                                           ROUND_UNITS[rnd])
        gather_cross(7, ag_all.at[slot], ROUND_UNITS[rnd + 1])
        gather_pair(8, ag_all.at[slot])
        whole = jnp.concatenate([ag_all[slot, s % 2, s // 2] for s in range(groups)], axis=-1)
        return jnp.concatenate([whole, jnp.zeros((ROWS - TOKENS, width), jnp.float32)], axis=0)

    for c in small:
        c.wait()
    h_ref[...] = jnp.concatenate(
        [x_vm[...].astype(jnp.float32), jnp.zeros((ROWS - batch, width), jnp.float32)], axis=0)

    new_rows = []
    for layer in range(layers):
        rnd = layer * ROUNDS
        base = layer * per_layer
        lhs[...] = rms_norm(h_ref[...], ng[layer, 0:1, :]).astype(jnp.bfloat16)
        stream(base, 3)
        q = rope_rotate(rms_norm(pick(acc[0]), qkg[layer, 0:1, :]), layer).astype(jnp.bfloat16)
        q_all[layer, core, chip] = q
        q = q.astype(jnp.float32)
        gather_cross(0, q_all.at[layer], ROUND_UNITS[rnd])
        gather_pair(1, q_all.at[layer])
        k_new = rope_rotate(rms_norm(pick(acc[1]), qkg[layer, 1:2, :]), layer).astype(jnp.bfloat16).astype(jnp.float32)
        v_new = pick(acc[2]).astype(jnp.bfloat16).astype(jnp.float32)
        new_rows.append((k_new, v_new))
        scale = head_dim ** -0.5
        s_new = jnp.sum(q * k_new, axis=-1, keepdims=True) * scale
        kv_copies[2 * layer].wait()
        kv_copies[2 * layer + 1].wait()
        q64 = jnp.concatenate([q_all[layer, s % 2, s // 2].astype(jnp.float32) for s in range(groups)], axis=0).astype(jnp.bfloat16)
        scores = jnp.zeros((ROWS, seq_dev * heads), jnp.float32)
        for b in range(batch):
            s = lax.dot_general(q64, kv[2 * layer, b], (((1,), (1,)), ((), ())), preferred_element_type=jnp.float32)
            s = jnp.where(hits[b], s, 0.0)
            for d in range(groups):
                scores = scores + s[d * ROWS:(d + 1) * ROWS]
        valid = paired
        if layer == 0:
            valid = valid & (me * seq_dev + wide_col // heads >= seq + 1 - WINDOW)
        scores = jnp.where(valid, scores * scale, NEG)
        m_loc = fold(scores, jnp.maximum)
        m_loc = jnp.where(own, jnp.maximum(m_loc, s_new), m_loc)
        ex = jnp.where(valid, jnp.exp(scores - jnp.tile(m_loc, (1, col_tiles))), 0.0)
        l_loc = fold(ex, jnp.add)
        l_loc = jnp.where(own, l_loc + jnp.exp(s_new - m_loc), l_loc)
        mine = lane // heads == row
        st_all[layer, me] = jnp.concatenate(
            [jnp.sum(jnp.where(mine, t, 0.0), axis=0, keepdims=True) for t in (m_loc, l_loc)], axis=0)
        got = start_round(2, [(st_all.at[layer, me], st_all.at[layer, me], (me + k) % groups) for k in range(1, groups)],
                          st_all.at[layer, pl.ds(0, groups - 1)])
        bulk(ROUND_UNITS[rnd + 1])
        got.wait_recv()
        def unpack(s, n):
            return fold(jnp.where(mine, jnp.broadcast_to(st_all[layer, s, n:n + 1, :], (ROWS, LANES)), 0.0), jnp.add)

        ms = [unpack(s, 0) for s in range(groups)]
        ls = [unpack(s, 1) for s in range(groups)]
        m_all = functools.reduce(jnp.maximum, ms)
        l_all = functools.reduce(jnp.add, [l * jnp.exp(m - m_all) for m, l in zip(ms, ls)])
        l_all = jnp.where(row < 2 * batch, jnp.maximum(l_all, 1e-30), 1.0)
        prob = jnp.where(valid, jnp.exp(scores - jnp.tile(m_all, (1, col_tiles))) / jnp.tile(l_all, (1, col_tiles)), 0.0)
        p_new = jnp.where(own & (lane < heads), jnp.exp(jnp.minimum(s_new - m_all, 0.0)) / l_all, 0.0)
        p_new = jnp.sum(p_new, axis=-1, keepdims=True).astype(jnp.bfloat16).astype(jnp.float32)
        prob64 = jnp.concatenate([prob] * groups, axis=0)
        weighted = jnp.zeros((groups * ROWS, head_dim), jnp.float32)
        for b in range(batch):
            weighted = weighted + jnp.dot(jnp.where(hits[b], prob64, 0.0).astype(jnp.bfloat16), kv[2 * layer + 1, b],
                                          preferred_element_type=jnp.float32)
        for d in range(groups):
            o_part[layer, d % 2, d // 2] = weighted[d * ROWS:(d + 1) * ROWS]
        o = scatter(3, o_part.at[layer], o_pair.at[layer], o_sum.at[layer], o_cross.at[layer], ROUND_UNITS[rnd + 2])
        o = o + p_new * v_new
        o = o.astype(jnp.bfloat16).astype(jnp.float32)
        o = jnp.concatenate([jnp.where(even, o, 0.0), jnp.where(even, 0.0, o)], axis=-1).astype(jnp.bfloat16)
        wo_copies[layer].wait()
        piece = width // groups
        for d in range(groups):
            y = jnp.dot(o, wo_buf[:, d * piece:(d + 1) * piece], preferred_element_type=jnp.float32)
            part[2 * layer, d % 2, d // 2] = merge(y)[:TOKENS]
        if layer + 1 < layers:
            wo_copies[layer + 1].start()
        hidden = h_ref[...] + rms_norm(all_reduce(rnd + 3, 2 * layer), ng[layer, 1:2, :])
        h_ref[...] = hidden
        lhs[...] = rms_norm(hidden, ng[layer, 2:3, :]).astype(jnp.bfloat16)
        stream(base + 3, 2 * ff_items)
        for n in range(ff_items):
            lhs[:, n * CHUNK:(n + 1) * CHUNK] = (
                jax.nn.gelu(acc[2 * n], approximate=True) * acc[2 * n + 1]).astype(jnp.bfloat16)
        stream(base + 3 + 2 * ff_items, wd_items)
        full = jnp.concatenate([acc[n] for n in range(wd_items)], axis=-1)
        for d in range(groups):
            part[2 * layer + 1, d % 2, d // 2] = full[:TOKENS, d * piece:(d + 1) * piece]
        hidden = h_ref[...] + rms_norm(all_reduce(rnd + 5, 2 * layer + 1), ng[layer, 3:4, :])
        h_ref[...] = hidden.astype(jnp.bfloat16).astype(jnp.float32)

    bulk(len(queue))
    for b in range(batch):
        h_out[b:b + 1, :] = h_ref[b:b + 1, :].astype(jnp.bfloat16)
    zeros = jnp.zeros((NEW_SLOTS - 1, 2, 2, LANES), jnp.bfloat16)
    for c in (2, 3):
        for b in range(batch):
            cache_out[c][b, seq + 1:] = zeros
    for step in list(pending):
        finish_sends(step)
    for c in range(4):
        own_rows = cache_out[c].at[0:batch, pl.ds(me * seq_dev, seq_dev)]
        pltpu.make_async_copy(own_rows, own_rows, self_sem.at[c]).wait()
        region = cache_out[c].at[0:batch, pl.ds(0, seq - seq_dev)]
        whole = pltpu.make_async_remote_copy(region, region, bulk_send.at[c], bulk_recv.at[c],
                                             device_id={"tp": sibling}, device_id_type=MESH)
        whole.wait_recv()
        whole.wait_send()
    slots = (seq % WINDOW, seq)
    for layer in range(layers):
        for n in range(2):
            for b in range(batch):
                for ct in range(2):
                    cache_out[2 * layer + n][b, slots[layer], ct] = new_rows[layer][n][
                        2 * b:2 * b + 2, ct * LANES:(ct + 1) * LANES].astype(jnp.bfloat16)


def flush_kernel(*refs):
    n = (len(refs) - 1) // 2
    copies = [pltpu.make_async_copy(refs[i], refs[n + i], refs[-1].at[i]) for i in range(n)]
    for c in copies:
        c.start()
    for c in copies:
        c.wait()


def solution(mesh):
    groups = mesh.shape["tp"]
    cache_in = P("dp", "tp", None, None)
    cache_out = P("dp", None, "tp", None)
    token_spec = P("dp", None)
    col_split = P(None, None, "tp")
    row_split = P(None, "tp", None)
    replicated = P()

    def per_device(k_local, v_local, k_global, v_global, x_token, w_q, w_k, w_v, w_o, w_gate, w_up, w_down, norm_gain, qk_gain):
        batch, seq_dev, heads, head_dim = k_local.shape
        layers, width, _ = w_q.shape
        ff_dev = w_gate.shape[2]
        seq = seq_dev * groups
        tiles, pairs, cols = heads // 8, 4, head_dim // LANES
        caches = (k_local, v_local, k_global, v_global)
        views = [c.reshape(batch, seq_dev, tiles, pairs, 2, cols, LANES).transpose(0, 1, 2, 5, 3, 4, 6) for c in caches]
        flat = [c.reshape(batch, seq_dev * heads, head_dim) for c in caches]
        inv_freq = [b ** (-2.0 * np.arange(head_dim // 2) / head_dim) for b in ROPE_BASES]
        angles = [seq / s * f for s, f in zip(POS_SCALES, inv_freq)]
        rope = jnp.asarray(np.stack([np.stack([np.cos(a), np.sin(a)]) for a in angles]), jnp.float32)
        any_spec = pl.BlockSpec(memory_space=pl.ANY)
        vmem_spec = pl.BlockSpec(memory_space=pltpu.VMEM)
        cfg = (groups, layers, batch, seq_dev, heads, head_dim, width, ff_dev)
        slots = (WINDOW, WINDOW, seq + NEW_SLOTS, seq + NEW_SLOTS)
        piece = width // groups
        chips = groups // 2
        res = pl.pallas_call(
            functools.partial(kernel, cfg),
            in_specs=[any_spec] * 19,
            out_specs=[vmem_spec] * 5,
            out_shape=[pltpu.VMEM((batch, s, 2, 2, LANES), jnp.bfloat16) for s in slots]
            + [pltpu.VMEM((batch, width), jnp.bfloat16)],
            scratch_shapes=[
                pltpu.VMEM((RING, width, CHUNK), jnp.bfloat16),
                pltpu.VMEM((w_o.shape[1], width), jnp.bfloat16),
                pltpu.VMEM((4, batch, seq_dev * heads, head_dim), jnp.bfloat16),
                pltpu.VMEM(x_token.shape, jnp.bfloat16),
                pltpu.VMEM(norm_gain.shape, jnp.float32),
                pltpu.VMEM(qk_gain.shape, jnp.float32),
                pltpu.VMEM(rope.shape, jnp.float32),
                pltpu.VMEM((ROWS, width), jnp.float32),
                pltpu.VMEM((ROWS, width), jnp.bfloat16),
                pltpu.VMEM((2 * ff_dev // CHUNK, ROWS, CHUNK), jnp.float32),
                pltpu.VMEM((layers, 2, chips, ROWS, head_dim), jnp.bfloat16),
                pltpu.VMEM((layers, groups, 2, LANES), jnp.float32),
                pltpu.VMEM((layers, 2, chips, ROWS, head_dim), jnp.float32),
                *[pltpu.VMEM((layers, chips, ROWS, head_dim), jnp.float32)] * 3,
                pltpu.VMEM((2 * layers, 2, chips, TOKENS, piece), jnp.float32),
                *[pltpu.VMEM((2 * layers, chips, TOKENS, piece), jnp.float32)] * 3,
                pltpu.VMEM((2 * layers, 2, chips, TOKENS, piece), jnp.float32),
                pltpu.SemaphoreType.DMA((RING,)),
                pltpu.SemaphoreType.DMA((layers,)),
                pltpu.SemaphoreType.DMA((4,)),
                pltpu.SemaphoreType.DMA((4,)),
                pltpu.SemaphoreType.DMA((4,)),
                pltpu.SemaphoreType.DMA((4,)),
                pltpu.SemaphoreType.DMA((4,)),
                pltpu.SemaphoreType.DMA((STEPS,)),
                pltpu.SemaphoreType.DMA((STEPS,)),
            ],
            compiler_params=pltpu.CompilerParams(
                collective_id=0, has_side_effects=True, vmem_limit_bytes=44 * 1024 * 1024),
        )(*views, *flat, x_token, w_q, w_k, w_v, w_o, w_gate, w_up, w_down, norm_gain, qk_gain, rope)
        held = [pltpu.with_memory_space_constraint(y, pltpu.VMEM) for y in res]
        res = pl.pallas_call(
            flush_kernel,
            in_specs=[vmem_spec] * 5,
            out_specs=[any_spec] * 5,
            out_shape=[jax.ShapeDtypeStruct(y.shape, y.dtype) for y in res],
            scratch_shapes=[pltpu.SemaphoreType.DMA((5,))],
            compiler_params=pltpu.CompilerParams(has_side_effects=True, vmem_limit_bytes=1024 * 1024),
        )(*held)
        outs = [y.transpose(0, 1, 3, 2, 4).reshape(batch, y.shape[1], 2, head_dim) for y in res[:4]]
        return (res[4], *outs)

    return jax.shard_map(per_device, mesh=mesh, in_specs=(cache_in, cache_in, cache_in, cache_in, token_spec, col_split, col_split, col_split, row_split, col_split, col_split, row_split, replicated, replicated), out_specs=(token_spec, cache_out, cache_out, cache_out, cache_out), check_vma=False)
```

```python
import functools

import jax
import jax.numpy as jnp
import numpy as np
from jax import lax
from jax.experimental import pallas as pl
from jax.experimental.pallas import tpu as pltpu
from jax.sharding import PartitionSpec as P

WINDOW = 1024
NEW_SLOTS = 128
NORM_EPS = 1e-6
ROPE_BASES = (10000.0, 1000000.0)
POS_SCALES = (1.0, 8.0)
NEG = -3.0e38
MESH = pl.DeviceIdType.MESH
LANES = 128
ROWS = 8
RING = 8
CHUNK = 512
SPLITS = 4
FIRST_UNITS = 4
ROUND_UNITS = (2, 2, 2, 2, 6, 2, 2, 2, 2, 2, 2, 6, 2, 2)
ROUNDS = 7
STEPS = 9


def rms_norm(values, gain_vec):
    mean_sq = jnp.mean(values * values, axis=-1, keepdims=True)
    return values * lax.rsqrt(mean_sq + NORM_EPS) * (1.0 + gain_vec)


def kernel(cfg, *refs):
    groups, layers, batch, seq_dev, heads, head_dim, width, ff_dev = cfg
    n_in, n_out = 2 * len(range(4)) + 11, 5
    ins, outs, scr = refs[:n_in], refs[n_in:n_in + n_out], refs[n_in + n_out:]
    views, caches = ins[:4], ins[4:8]
    x_hbm, wq, wk, wv, wo, wg, wu, wd, ng_hbm, qk_hbm, rope_hbm = ins[8:]
    cache_out, h_out = outs[:4], outs[4]
    (ring, wo_buf, kv, x_vm, ng, qkg, rope, h_ref, lhs, acc, q_all, st_all, o_part, o_pair, o_sum, o_cross,
     part, rs_pair, rs_sum, rs_cross, ag_all,
     ring_sem, wo_sem, kv_sem, small_sem, self_sem, bulk_send, bulk_recv, r_send, r_recv) = scr
    me = lax.axis_index("tp")
    per_tile = heads // 2
    pairs = per_tile // 2
    seq = seq_dev * groups
    half_dim = head_dim // 2
    ff_items = ff_dev // CHUNK
    wd_items = width // CHUNK
    per_layer = 3 + 2 * ff_items + wd_items
    items = layers * per_layer

    def issue(item):
        item = jnp.asarray(item, jnp.int32)
        layer = item // per_layer
        r = item % per_layer
        slot = item % RING
        dst = ring.at[slot]
        sem = ring_sem.at[slot]
        for pos, ref in enumerate((wq, wk, wv)):
            @pl.when(r == pos)
            def _(ref=ref):
                pltpu.make_async_copy(ref.at[layer], dst, sem).start()
        for par, ref in enumerate((wg, wu)):
            @pl.when((r >= 3) & (r < 3 + 2 * ff_items) & ((r - 3) % 2 == par))
            def _(ref=ref):
                col = pl.multiple_of(jnp.clip((r - 3) // 2, 0, ff_items - 1) * CHUNK, CHUNK)
                pltpu.make_async_copy(ref.at[layer, :, pl.ds(col, CHUNK)], dst, sem).start()

        @pl.when(r >= 3 + 2 * ff_items)
        def _():
            col = pl.multiple_of(jnp.clip(r - 3 - 2 * ff_items, 0, wd_items - 1) * CHUNK, CHUNK)
            pltpu.make_async_copy(wd.at[layer, :, pl.ds(col, CHUNK)], dst, sem).start()

    def stream(first, count):
        def step(t, carry):
            item = first + t
            slot = item % RING
            pltpu.make_async_copy(wq.at[0], ring.at[slot], ring_sem.at[slot]).wait()
            acc[t] = jnp.dot(lhs[...], ring[slot], preferred_element_type=jnp.float32)

            @pl.when(item + RING < items)
            def _():
                issue(item + RING)
            return carry
        lax.fori_loop(0, count, step, 0)

    barrier = pltpu.get_barrier_semaphore()
    for k in range(1, groups):
        pl.semaphore_signal(barrier, inc=1, device_id={"tp": (me + k) % groups}, device_id_type=MESH)
    small = [pltpu.make_async_copy(s, d, small_sem.at[n]) for n, (s, d) in enumerate(
        ((x_hbm, x_vm), (ng_hbm, ng), (qk_hbm, qkg), (rope_hbm, rope)))]
    for c in small:
        c.start()
    for n in range(3):
        issue(n)
    kv_copies = [pltpu.make_async_copy(caches[n], kv.at[n], kv_sem.at[n]) for n in range(4)]
    wo_copies = [pltpu.make_async_copy(wo.at[n], wo_buf, wo_sem.at[n]) for n in range(layers)]
    kv_copies[0].start()
    kv_copies[1].start()
    wo_copies[0].start()
    for n in range(3, RING):
        issue(n)

    pl.semaphore_wait(barrier, groups - 1)

    span = seq_dev // SPLITS
    units = [(c, b, f) for c in range(4) for b in range(batch) for f in range(SPLITS)]
    chips = groups // 2
    order = [(dx, dc) for dc in range(2) for dx in (1, chips - 1, *range(2, chips - 1))] + [(0, 1)]
    chip, core = me // 2, me % 2

    def peer(dx, dc):
        return ((chip + dx) % chips) * 2 + (core + dc) % 2

    def view_of(c, owner, b, start, size):
        return views[c].at[b, pl.ds(start, size), owner // pairs, :, owner % pairs]

    queue = list(units)

    def bulk(count):
        for _ in range(min(count, len(queue))):
            c, b, f = queue.pop(0)
            for k, (dx, dc) in enumerate(order):
                dst = peer(dx, dc)
                pltpu.make_async_remote_copy(
                    view_of(c, dst, b, f * span, span),
                    cache_out[c].at[b, pl.ds(me * seq_dev + f * span, span)],
                    bulk_send.at[c], bulk_recv.at[c],
                    device_id={"tp": dst}, device_id_type=MESH).start()

    bulk(FIRST_UNITS)
    self_copies = [pltpu.make_async_copy(
        view_of(c, me, b, 0, seq_dev), cache_out[c].at[b, pl.ds(me * seq_dev, seq_dev)], self_sem.at[c])
        for c in range(4) for b in range(batch)]
    for c in self_copies:
        c.start()
    kv_copies[2].start()
    kv_copies[3].start()

    sibling = chip * 2 + 1 - core
    pending = {}

    def start_round(step, copies, size_of):
        finish_sends(step)
        for src, dst, device in copies:
            pltpu.make_async_remote_copy(src, dst, r_send.at[step], r_recv.at[step],
                                         device_id={"tp": device}, device_id_type=MESH).start()
        pending[step] = pltpu.make_async_remote_copy(size_of, size_of, r_send.at[step], r_recv.at[step],
                                                     device_id={"tp": sibling}, device_id_type=MESH)
        return pending[step]

    def finish_sends(step):
        if step in pending:
            pending.pop(step).wait_send()

    others = [(chip + dx) % chips for dx in (1, chips - 1, *range(2, chips - 1))]

    def gather_cross(step, ref, units):
        got = start_round(step, [(ref.at[core, chip], ref.at[core, chip], t * 2 + core) for t in others],
                          ref.at[core, pl.ds(0, chips - 1)])
        bulk(units)
        got.wait_recv()

    def gather_pair(step, ref):
        start_round(step, [(ref.at[core], ref.at[core], sibling)], ref.at[core]).wait_recv()

    def scatter(step, mine, pair, summed, cross, units):
        start_round(step, [(mine.at[1 - core], pair, sibling)], pair).wait_recv()
        for t in range(chips):
            summed[t] = mine[core, t] + pair[t]
        got = start_round(step + 1, [(summed.at[t], cross.at[chip], t * 2 + core) for t in others],
                          cross.at[pl.ds(0, chips - 1)])
        bulk(units)
        cross[chip] = summed[chip]
        got.wait_recv()
        total = cross[0]
        for t in range(1, chips):
            total = total + cross[t]
        return total

    row = lax.broadcasted_iota(jnp.int32, (ROWS, LANES), 0)
    lane = lax.broadcasted_iota(jnp.int32, (ROWS, LANES), 1)
    even = lax.broadcasted_iota(jnp.int32, (ROWS, 1), 0) % 2 == 0
    lane_head = lane % heads
    own = (lane_head == 2 * me + row % 2) & (row < 2 * batch)
    col_tiles = seq_dev * heads // LANES
    row64 = lax.broadcasted_iota(jnp.int32, (groups * ROWS, LANES), 0)
    lane64 = lax.broadcasted_iota(jnp.int32, (groups * ROWS, LANES), 1)
    head_hit = (lane64 % heads) == 2 * (row64 // ROWS) + row64 % 2
    hits = [jnp.tile(head_hit & ((row64 % ROWS) // 2 == b), (1, col_tiles)) for b in range(batch)]
    wide_row = lax.broadcasted_iota(jnp.int32, (ROWS, seq_dev * heads), 0)
    wide_col = lax.broadcasted_iota(jnp.int32, (ROWS, seq_dev * heads), 1)
    paired = (wide_col % 2 == wide_row % 2) & (wide_row < 2 * batch)

    def fold(x, op):
        out = x[:, :LANES]
        for n in range(1, x.shape[1] // LANES):
            out = op(out, x[:, n * LANES:(n + 1) * LANES])
        shift = heads
        while shift < LANES:
            out = op(out, pltpu.roll(out, shift, 1))
            shift *= 2
        return out

    def rope_rotate(x, layer):
        cos, sin = rope[layer, 0:1, :], rope[layer, 1:2, :]
        a, b = x[:, :half_dim], x[:, half_dim:]
        return jnp.concatenate([a * cos - b * sin, b * cos + a * sin], axis=-1)

    row1 = lax.broadcasted_iota(jnp.int32, (ROWS, 1), 0)

    def pick(y):
        y = jnp.where(row1 == 0, y, jnp.where(row1 < 3, pltpu.roll(y, 1, 0), jnp.where(
            row1 < 5, pltpu.roll(y, 2, 0), pltpu.roll(y, 3, 0))))
        return jnp.where(even, y[:, :head_dim], y[:, head_dim:])

    def pair_rows(y):
        return jnp.concatenate([*(y[b] for b in range(batch)), jnp.zeros((ROWS - 2 * batch, head_dim), jnp.float32)], axis=0)

    def merge(y):
        y = y + pltpu.roll(y, ROWS - 1, 0)
        return jnp.where(row1 == 0, y, jnp.where(row1 == 1, pltpu.roll(y, ROWS - 1, 0), jnp.where(
            row1 == 2, pltpu.roll(y, ROWS - 2, 0), 0.0)))

    def all_reduce(rnd, slot):
        ag_all[slot, core, chip] = scatter(5, part.at[slot], rs_pair.at[slot], rs_sum.at[slot], rs_cross.at[slot],
                                           ROUND_UNITS[rnd])
        gather_cross(7, ag_all.at[slot], ROUND_UNITS[rnd + 1])
        gather_pair(8, ag_all.at[slot])
        whole = [jnp.concatenate([ag_all[slot, s % 2, s // 2, b] for s in range(groups)], axis=-1) for b in range(batch)]
        return jnp.concatenate([*whole, jnp.zeros((ROWS - batch, width), jnp.float32)], axis=0)

    for c in small:
        c.wait()
    h_ref[...] = jnp.concatenate(
        [x_vm[...].astype(jnp.float32), jnp.zeros((ROWS - batch, width), jnp.float32)], axis=0)

    new_rows = []
    for layer in range(layers):
        rnd = layer * ROUNDS
        base = layer * per_layer
        lhs[...] = rms_norm(h_ref[...], ng[layer, 0:1, :]).astype(jnp.bfloat16)
        stream(base, 3)
        q = rope_rotate(rms_norm(pick(acc[0]), qkg[layer, 0:1, :]), layer).astype(jnp.bfloat16).astype(jnp.float32)
        for b in range(batch):
            q_all[layer, core, chip, b] = q[2 * b:2 * b + 2].astype(jnp.bfloat16)
        gather_cross(0, q_all.at[layer], ROUND_UNITS[rnd])
        gather_pair(1, q_all.at[layer])
        k_new = rope_rotate(rms_norm(pick(acc[1]), qkg[layer, 1:2, :]), layer).astype(jnp.bfloat16).astype(jnp.float32)
        v_new = pick(acc[2]).astype(jnp.bfloat16).astype(jnp.float32)
        new_rows.append((k_new, v_new))
        scale = head_dim ** -0.5
        s_new = jnp.sum(q * k_new, axis=-1, keepdims=True) * scale
        kv_copies[2 * layer].wait()
        kv_copies[2 * layer + 1].wait()
        q64 = jnp.concatenate([pair_rows(q_all[layer, s % 2, s // 2].astype(jnp.float32)) for s in range(groups)], axis=0).astype(jnp.bfloat16)
        scores = jnp.zeros((ROWS, seq_dev * heads), jnp.float32)
        for b in range(batch):
            s = lax.dot_general(q64, kv[2 * layer, b], (((1,), (1,)), ((), ())), preferred_element_type=jnp.float32)
            s = jnp.where(hits[b], s, 0.0)
            for d in range(groups):
                scores = scores + s[d * ROWS:(d + 1) * ROWS]
        valid = paired
        if layer == 0:
            valid = valid & (me * seq_dev + wide_col // heads >= seq + 1 - WINDOW)
        scores = jnp.where(valid, scores * scale, NEG)
        m_loc = fold(scores, jnp.maximum)
        m_loc = jnp.where(own, jnp.maximum(m_loc, s_new), m_loc)
        ex = jnp.where(valid, jnp.exp(scores - jnp.tile(m_loc, (1, col_tiles))), 0.0)
        l_loc = fold(ex, jnp.add)
        l_loc = jnp.where(own, l_loc + jnp.exp(s_new - m_loc), l_loc)
        mine = lane // heads == row
        st_all[layer, me] = jnp.concatenate(
            [jnp.sum(jnp.where(mine, t, 0.0), axis=0, keepdims=True) for t in (m_loc, l_loc)], axis=0)
        got = start_round(2, [(st_all.at[layer, me], st_all.at[layer, me], (me + k) % groups) for k in range(1, groups)],
                          st_all.at[layer, pl.ds(0, groups - 1)])
        bulk(ROUND_UNITS[rnd + 1])
        got.wait_recv()
        def unpack(s, n):
            return fold(jnp.where(mine, jnp.broadcast_to(st_all[layer, s, n:n + 1, :], (ROWS, LANES)), 0.0), jnp.add)

        ms = [unpack(s, 0) for s in range(groups)]
        ls = [unpack(s, 1) for s in range(groups)]
        m_all = functools.reduce(jnp.maximum, ms)
        l_all = functools.reduce(jnp.add, [l * jnp.exp(m - m_all) for m, l in zip(ms, ls)])
        l_all = jnp.where(row < 2 * batch, jnp.maximum(l_all, 1e-30), 1.0)
        prob = jnp.where(valid, jnp.exp(scores - jnp.tile(m_all, (1, col_tiles))) / jnp.tile(l_all, (1, col_tiles)), 0.0)
        p_new = jnp.where(own & (lane < heads), jnp.exp(jnp.minimum(s_new - m_all, 0.0)) / l_all, 0.0)
        p_new = jnp.sum(p_new, axis=-1, keepdims=True).astype(jnp.bfloat16).astype(jnp.float32)
        prob64 = jnp.concatenate([prob] * groups, axis=0)
        weighted = jnp.zeros((groups * ROWS, head_dim), jnp.float32)
        for b in range(batch):
            weighted = weighted + jnp.dot(jnp.where(hits[b], prob64, 0.0).astype(jnp.bfloat16), kv[2 * layer + 1, b],
                                          preferred_element_type=jnp.float32)
        for d in range(groups):
            for b in range(batch):
                o_part[layer, d % 2, d // 2, b] = weighted[d * ROWS + 2 * b:d * ROWS + 2 * b + 2]
        o = scatter(3, o_part.at[layer], o_pair.at[layer], o_sum.at[layer], o_cross.at[layer], ROUND_UNITS[rnd + 2])
        o = pair_rows(o) + p_new * v_new
        o = o.astype(jnp.bfloat16).astype(jnp.float32)
        o = jnp.concatenate([jnp.where(even, o, 0.0), jnp.where(even, 0.0, o)], axis=-1).astype(jnp.bfloat16)
        wo_copies[layer].wait()
        piece = width // groups
        for d in range(groups):
            y = jnp.dot(o, wo_buf[:, d * piece:(d + 1) * piece], preferred_element_type=jnp.float32)
            y = merge(y)
            for b in range(batch):
                part[2 * layer, d % 2, d // 2, b] = y[b:b + 1]
        if layer + 1 < layers:
            wo_copies[layer + 1].start()
        hidden = h_ref[...] + rms_norm(all_reduce(rnd + 3, 2 * layer), ng[layer, 1:2, :])
        h_ref[...] = hidden
        lhs[...] = rms_norm(hidden, ng[layer, 2:3, :]).astype(jnp.bfloat16)
        stream(base + 3, 2 * ff_items)
        for n in range(ff_items):
            lhs[:, n * CHUNK:(n + 1) * CHUNK] = (
                jax.nn.gelu(acc[2 * n], approximate=True) * acc[2 * n + 1]).astype(jnp.bfloat16)
        stream(base + 3 + 2 * ff_items, wd_items)
        full = jnp.concatenate([acc[n] for n in range(wd_items)], axis=-1)
        for d in range(groups):
            for b in range(batch):
                part[2 * layer + 1, d % 2, d // 2, b] = full[b:b + 1, d * piece:(d + 1) * piece]
        hidden = h_ref[...] + rms_norm(all_reduce(rnd + 5, 2 * layer + 1), ng[layer, 3:4, :])
        h_ref[...] = hidden.astype(jnp.bfloat16).astype(jnp.float32)

    bulk(len(queue))
    for b in range(batch):
        h_out[b:b + 1, :] = h_ref[b:b + 1, :].astype(jnp.bfloat16)
    zeros = jnp.zeros((NEW_SLOTS - 1, 2, 2, LANES), jnp.bfloat16)
    for c in (2, 3):
        for b in range(batch):
            cache_out[c][b, seq + 1:] = zeros
    for step in list(pending):
        finish_sends(step)
    for c in range(4):
        own_rows = cache_out[c].at[0:batch, pl.ds(me * seq_dev, seq_dev)]
        pltpu.make_async_copy(own_rows, own_rows, self_sem.at[c]).wait()
        region = cache_out[c].at[0:batch, pl.ds(0, seq - seq_dev)]
        whole = pltpu.make_async_remote_copy(region, region, bulk_send.at[c], bulk_recv.at[c],
                                             device_id={"tp": sibling}, device_id_type=MESH)
        whole.wait_recv()
        whole.wait_send()
    slots = (seq % WINDOW, seq)
    for layer in range(layers):
        for n in range(2):
            for b in range(batch):
                for ct in range(2):
                    cache_out[2 * layer + n][b, slots[layer], ct] = new_rows[layer][n][
                        2 * b:2 * b + 2, ct * LANES:(ct + 1) * LANES].astype(jnp.bfloat16)


def flush_kernel(*refs):
    n = (len(refs) - 1) // 2
    copies = [pltpu.make_async_copy(refs[i], refs[n + i], refs[-1].at[i]) for i in range(n)]
    for c in copies:
        c.start()
    for c in copies:
        c.wait()


def solution(mesh):
    groups = mesh.shape["tp"]
    cache_in = P("dp", "tp", None, None)
    cache_out = P("dp", None, "tp", None)
    token_spec = P("dp", None)
    col_split = P(None, None, "tp")
    row_split = P(None, "tp", None)
    replicated = P()

    def per_device(k_local, v_local, k_global, v_global, x_token, w_q, w_k, w_v, w_o, w_gate, w_up, w_down, norm_gain, qk_gain):
        batch, seq_dev, heads, head_dim = k_local.shape
        layers, width, _ = w_q.shape
        ff_dev = w_gate.shape[2]
        seq = seq_dev * groups
        tiles, pairs, cols = heads // 8, 4, head_dim // LANES
        caches = (k_local, v_local, k_global, v_global)
        views = [c.reshape(batch, seq_dev, tiles, pairs, 2, cols, LANES).transpose(0, 1, 2, 5, 3, 4, 6) for c in caches]
        flat = [c.reshape(batch, seq_dev * heads, head_dim) for c in caches]
        inv_freq = [b ** (-2.0 * np.arange(head_dim // 2) / head_dim) for b in ROPE_BASES]
        angles = [seq / s * f for s, f in zip(POS_SCALES, inv_freq)]
        rope = jnp.asarray(np.stack([np.stack([np.cos(a), np.sin(a)]) for a in angles]), jnp.float32)
        any_spec = pl.BlockSpec(memory_space=pl.ANY)
        vmem_spec = pl.BlockSpec(memory_space=pltpu.VMEM)
        cfg = (groups, layers, batch, seq_dev, heads, head_dim, width, ff_dev)
        slots = (WINDOW, WINDOW, seq + NEW_SLOTS, seq + NEW_SLOTS)
        piece = width // groups
        chips = groups // 2
        res = pl.pallas_call(
            functools.partial(kernel, cfg),
            in_specs=[any_spec] * 19,
            out_specs=[vmem_spec] * 5,
            out_shape=[pltpu.VMEM((batch, s, 2, 2, LANES), jnp.bfloat16) for s in slots]
            + [pltpu.VMEM((batch, width), jnp.bfloat16)],
            scratch_shapes=[
                pltpu.VMEM((RING, width, CHUNK), jnp.bfloat16),
                pltpu.VMEM((w_o.shape[1], width), jnp.bfloat16),
                pltpu.VMEM((4, batch, seq_dev * heads, head_dim), jnp.bfloat16),
                pltpu.VMEM(x_token.shape, jnp.bfloat16),
                pltpu.VMEM(norm_gain.shape, jnp.float32),
                pltpu.VMEM(qk_gain.shape, jnp.float32),
                pltpu.VMEM(rope.shape, jnp.float32),
                pltpu.VMEM((ROWS, width), jnp.float32),
                pltpu.VMEM((ROWS, width), jnp.bfloat16),
                pltpu.VMEM((2 * ff_dev // CHUNK, ROWS, CHUNK), jnp.float32),
                pltpu.VMEM((layers, 2, chips, batch, 2, head_dim), jnp.bfloat16),
                pltpu.VMEM((layers, groups, 2, LANES), jnp.float32),
                pltpu.VMEM((layers, 2, chips, batch, 2, head_dim), jnp.float32),
                *[pltpu.VMEM((layers, chips, batch, 2, head_dim), jnp.float32)] * 3,
                pltpu.VMEM((2 * layers, 2, chips, batch, 1, piece), jnp.float32),
                *[pltpu.VMEM((2 * layers, chips, batch, 1, piece), jnp.float32)] * 3,
                pltpu.VMEM((2 * layers, 2, chips, batch, 1, piece), jnp.float32),
                pltpu.SemaphoreType.DMA((RING,)),
                pltpu.SemaphoreType.DMA((layers,)),
                pltpu.SemaphoreType.DMA((4,)),
                pltpu.SemaphoreType.DMA((4,)),
                pltpu.SemaphoreType.DMA((4,)),
                pltpu.SemaphoreType.DMA((4,)),
                pltpu.SemaphoreType.DMA((4,)),
                pltpu.SemaphoreType.DMA((STEPS,)),
                pltpu.SemaphoreType.DMA((STEPS,)),
            ],
            compiler_params=pltpu.CompilerParams(
                collective_id=0, has_side_effects=True, vmem_limit_bytes=44 * 1024 * 1024),
        )(*views, *flat, x_token, w_q, w_k, w_v, w_o, w_gate, w_up, w_down, norm_gain, qk_gain, rope)
        held = [pltpu.with_memory_space_constraint(y, pltpu.VMEM) for y in res]
        res = pl.pallas_call(
            flush_kernel,
            in_specs=[vmem_spec] * 5,
            out_specs=[any_spec] * 5,
            out_shape=[jax.ShapeDtypeStruct(y.shape, y.dtype) for y in res],
            scratch_shapes=[pltpu.SemaphoreType.DMA((5,))],
            compiler_params=pltpu.CompilerParams(has_side_effects=True, vmem_limit_bytes=1024 * 1024),
        )(*held)
        outs = [y.transpose(0, 1, 3, 2, 4).reshape(batch, y.shape[1], 2, head_dim) for y in res[:4]]
        return (res[4], *outs)

    return jax.shard_map(per_device, mesh=mesh, in_specs=(cache_in, cache_in, cache_in, cache_in, token_spec, col_split, col_split, col_split, row_split, col_split, col_split, row_split, replicated, replicated), out_specs=(token_spec, cache_out, cache_out, cache_out, cache_out), check_vma=False)
```

```python
import functools

import jax
import jax.numpy as jnp
import numpy as np
from jax import lax
from jax.experimental import pallas as pl
from jax.experimental.pallas import tpu as pltpu
from jax.sharding import PartitionSpec as P

WINDOW = 1024
NEW_SLOTS = 128
NORM_EPS = 1e-6
ROPE_BASES = (10000.0, 1000000.0)
POS_SCALES = (1.0, 8.0)
NEG = -3.0e38
MESH = pl.DeviceIdType.MESH
LANES = 128
ROWS = 8
RING = 8
CHUNK = 512
SPLITS = 4
FIRST_UNITS = 6
ROUND_UNITS = (2, 2, 2, 2, 6, 2, 2, 2, 2, 2, 2, 6, 2, 2)
ROUNDS = 7


def rms_norm(values, gain_vec):
    mean_sq = jnp.mean(values * values, axis=-1, keepdims=True)
    return values * lax.rsqrt(mean_sq + NORM_EPS) * (1.0 + gain_vec)


def kernel(cfg, *refs):
    groups, layers, batch, seq_dev, heads, head_dim, width, ff_dev = cfg
    n_in, n_out = 2 * len(range(4)) + 11, 5
    ins, outs, scr = refs[:n_in], refs[n_in:n_in + n_out], refs[n_in + n_out:]
    views, caches = ins[:4], ins[4:8]
    x_hbm, wq, wk, wv, wo, wg, wu, wd, ng_hbm, qk_hbm, rope_hbm = ins[8:]
    cache_out, h_out = outs[:4], outs[4]
    (ring, wo_buf, kv, x_vm, ng, qkg, rope, h_ref, lhs, acc, q_all, st_all, o_part, o_pair, o_sum, o_cross,
     part, rs_pair, rs_sum, rs_cross, ag_all,
     ring_sem, local_sem, bulk_sem, r_send, r_recv) = scr
    me = lax.axis_index("tp")
    per_tile = heads // 2
    pairs = per_tile // 2
    seq = seq_dev * groups
    half_dim = head_dim // 2
    ff_items = ff_dev // CHUNK
    wd_items = width // CHUNK
    per_layer = 3 + 2 * ff_items + wd_items
    items = layers * per_layer

    def issue(item):
        layer = item // per_layer
        r = item % per_layer
        slot = item % RING
        dst = ring.at[slot]
        sem = ring_sem.at[slot]
        for pos, ref in enumerate((wq, wk, wv)):
            @pl.when(r == pos)
            def _(ref=ref):
                pltpu.make_async_copy(ref.at[layer], dst, sem).start()
        for par, ref in enumerate((wg, wu)):
            @pl.when((r >= 3) & (r < 3 + 2 * ff_items) & ((r - 3) % 2 == par))
            def _(ref=ref):
                col = pl.multiple_of(jnp.clip((r - 3) // 2, 0, ff_items - 1) * CHUNK, CHUNK)
                pltpu.make_async_copy(ref.at[layer, :, pl.ds(col, CHUNK)], dst, sem).start()

        @pl.when(r >= 3 + 2 * ff_items)
        def _():
            col = pl.multiple_of(jnp.clip(r - 3 - 2 * ff_items, 0, wd_items - 1) * CHUNK, CHUNK)
            pltpu.make_async_copy(wd.at[layer, :, pl.ds(col, CHUNK)], dst, sem).start()

    def stream(first, count):
        def step(t, carry):
            item = first + t
            slot = item % RING
            pltpu.make_async_copy(wq.at[0], ring.at[slot], ring_sem.at[slot]).wait()
            acc[t] = jnp.dot(lhs[...], ring[slot], preferred_element_type=jnp.float32)

            @pl.when(item + RING < items)
            def _():
                issue(item + RING)
            return carry
        lax.fori_loop(0, count, step, 0)

    barrier = pltpu.get_barrier_semaphore()
    for k in range(1, groups):
        pl.semaphore_signal(barrier, inc=1, device_id={"tp": (me + k) % groups}, device_id_type=MESH)
    pl.semaphore_wait(barrier, groups - 1)

    span = seq_dev // SPLITS
    units = [(c, b, f) for c in range(4) for b in range(batch) for f in range(SPLITS)]
    chips = groups // 2
    order = [(dx, dc) for dc in range(2) for dx in (1, chips - 1, *range(2, chips - 1))] + [(0, 1)]
    chip, core = me // 2, me % 2

    def peer(dx, dc):
        return ((chip + dx) % chips) * 2 + (core + dc) % 2

    def view_of(c, owner, b, start, size):
        return views[c].at[b, pl.ds(start, size), owner // pairs, :, owner % pairs]

    queue = list(units)

    def bulk(count):
        for _ in range(min(count, len(queue))):
            c, b, f = queue.pop(0)
            for k, (dx, dc) in enumerate(order):
                dst = peer(dx, dc)
                pltpu.make_async_remote_copy(
                    view_of(c, dst, b, f * span, span),
                    cache_out[c].at[b, pl.ds(me * seq_dev + f * span, span)],
                    bulk_sem.at[0], bulk_sem.at[1],
                    device_id={"tp": dst}, device_id_type=MESH).start()

    bulk(FIRST_UNITS)
    def load(src, dst, which):
        c = pltpu.make_async_copy(src, dst, local_sem.at[which])
        c.start()
        return c

    SMALL, OUT, HEADS, SELF = range(4)
    small = ((x_hbm, x_vm), (ng_hbm, ng), (qk_hbm, qkg), (rope_hbm, rope))
    small_copies = [load(*small[0], SMALL)] + [load(*small[n], 3 + n) for n in (1, 2, 3)]
    for n in range(3):
        pltpu.make_async_copy((wq, wk, wv)[n].at[0], ring.at[n], ring_sem.at[n]).start()
    load(caches[0], kv.at[0], HEADS)
    load(caches[1], kv.at[1], HEADS)
    wo_copy = load(wo.at[0], wo_buf, OUT)
    for n in range(3, RING):
        issue(jnp.int32(n))
    for c in range(4):
        for b in range(batch):
            load(view_of(c, me, b, 0, seq_dev), cache_out[c].at[b, pl.ds(me * seq_dev, seq_dev)], SELF)

    sibling = chip * 2 + 1 - core
    turns = {"pair": 0, "cross": 0, "all": 0}
    pending = []

    def start_round(kind, copies, size_of):
        if len(pending) == 2:
            pending.pop(0).wait_send()
        turn = turns[kind]
        turns[kind] += 1
        s_sem = r_send.at[sum(turns.values()) % 2]
        r_sem = r_recv.at[{"pair": 0, "cross": 2, "all": 4}[kind] + (turn % 2 if kind != "all" else 0)]
        for src, dst, device in copies:
            pltpu.make_async_remote_copy(src, dst, s_sem, r_sem, device_id={"tp": device}, device_id_type=MESH).start()
        pending.append(pltpu.make_async_remote_copy(size_of, size_of, s_sem, r_sem,
                                                    device_id={"tp": sibling}, device_id_type=MESH))
        return pending[-1]

    others = [(chip + dx) % chips for dx in (1, chips - 1, *range(2, chips - 1))]

    def gather_cross(ref, units):
        got = start_round("cross", [(ref.at[core, chip], ref.at[core, chip], t * 2 + core) for t in others],
                          ref.at[core, pl.ds(0, chips - 1)])
        bulk(units)
        got.wait_recv()

    def gather_pair(ref):
        start_round("pair", [(ref.at[core], ref.at[core], sibling)], ref.at[core]).wait_recv()

    def scatter(mine, pair, summed, cross, units):
        start_round("pair", [(mine.at[1 - core], pair, sibling)], pair).wait_recv()
        for t in range(chips):
            summed[t] = mine[core, t] + pair[t]
        got = start_round("cross", [(summed.at[t], cross.at[chip], t * 2 + core) for t in others],
                          cross.at[pl.ds(0, chips - 1)])
        bulk(units)
        cross[chip] = summed[chip]
        got.wait_recv()
        total = cross[0]
        for t in range(1, chips):
            total = total + cross[t]
        return total

    row = lax.broadcasted_iota(jnp.int32, (ROWS, LANES), 0)
    lane = lax.broadcasted_iota(jnp.int32, (ROWS, LANES), 1)
    even = lax.broadcasted_iota(jnp.int32, (ROWS, 1), 0) % 2 == 0
    lane_head = lane % heads
    own = (lane_head == 2 * me + row % 2) & (row < 2 * batch)
    col_tiles = seq_dev * heads // LANES
    row64 = lax.broadcasted_iota(jnp.int32, (groups * ROWS, LANES), 0)
    lane64 = lax.broadcasted_iota(jnp.int32, (groups * ROWS, LANES), 1)
    head_hit = (lane64 % heads) == 2 * (row64 // ROWS) + row64 % 2
    hits = [jnp.tile(head_hit & ((row64 % ROWS) // 2 == b), (1, col_tiles)) for b in range(batch)]
    wide_row = lax.broadcasted_iota(jnp.int32, (ROWS, seq_dev * heads), 0)
    wide_col = lax.broadcasted_iota(jnp.int32, (ROWS, seq_dev * heads), 1)
    paired = (wide_col % 2 == wide_row % 2) & (wide_row < 2 * batch)

    def fold(x, op):
        out = x[:, :LANES]
        for n in range(1, x.shape[1] // LANES):
            out = op(out, x[:, n * LANES:(n + 1) * LANES])
        shift = heads
        while shift < LANES:
            out = op(out, pltpu.roll(out, shift, 1))
            shift *= 2
        return out

    def rope_rotate(x, layer):
        cos, sin = rope[layer, 0:1, :], rope[layer, 1:2, :]
        a, b = x[:, :half_dim], x[:, half_dim:]
        return jnp.concatenate([a * cos - b * sin, b * cos + a * sin], axis=-1)

    row1 = lax.broadcasted_iota(jnp.int32, (ROWS, 1), 0)

    def pick(y):
        y = jnp.where(row1 == 0, y, jnp.where(row1 < 3, pltpu.roll(y, 1, 0), jnp.where(
            row1 < 5, pltpu.roll(y, 2, 0), pltpu.roll(y, 3, 0))))
        return jnp.where(even, y[:, :head_dim], y[:, head_dim:])

    def pair_rows(y):
        return jnp.concatenate([*(y[b] for b in range(batch)), jnp.zeros((ROWS - 2 * batch, head_dim), jnp.float32)], axis=0)

    def merge(y):
        y = y + pltpu.roll(y, ROWS - 1, 0)
        return jnp.where(row1 == 0, y, jnp.where(row1 == 1, pltpu.roll(y, ROWS - 1, 0), jnp.where(
            row1 == 2, pltpu.roll(y, ROWS - 2, 0), 0.0)))

    def all_reduce(rnd, slot):
        ag_all[slot, core, chip] = scatter(part.at[slot], rs_pair.at[slot], rs_sum.at[slot], rs_cross.at[slot],
                                           ROUND_UNITS[rnd])
        gather_cross(ag_all.at[slot], ROUND_UNITS[rnd + 1])
        gather_pair(ag_all.at[slot])
        whole = [jnp.concatenate([ag_all[slot, s % 2, s // 2, b] for s in range(groups)], axis=-1) for b in range(batch)]
        return jnp.concatenate([*whole, jnp.zeros((ROWS - batch, width), jnp.float32)], axis=0)

    for c in small_copies:
        c.wait()
    h_ref[...] = jnp.concatenate(
        [x_vm[...].astype(jnp.float32), jnp.zeros((ROWS - batch, width), jnp.float32)], axis=0)

    new_rows = []
    for layer in range(layers):
        rnd = layer * ROUNDS
        base = layer * per_layer
        lhs[...] = rms_norm(h_ref[...], ng[layer, 0:1, :]).astype(jnp.bfloat16)
        stream(base, 3)
        q = rope_rotate(rms_norm(pick(acc[0]), qkg[layer, 0:1, :]), layer).astype(jnp.bfloat16).astype(jnp.float32)
        for b in range(batch):
            q_all[layer, core, chip, b] = q[2 * b:2 * b + 2].astype(jnp.bfloat16)
        gather_cross(q_all.at[layer], ROUND_UNITS[rnd])
        gather_pair(q_all.at[layer])
        k_new = rope_rotate(rms_norm(pick(acc[1]), qkg[layer, 1:2, :]), layer).astype(jnp.bfloat16).astype(jnp.float32)
        v_new = pick(acc[2]).astype(jnp.bfloat16).astype(jnp.float32)
        new_rows.append((k_new, v_new))
        scale = head_dim ** -0.5
        s_new = jnp.sum(q * k_new, axis=-1, keepdims=True) * scale
        both = kv.at[2 * layer:2 * layer + 2]
        pltpu.make_async_copy(both, both, local_sem.at[HEADS]).wait()
        if layer + 1 < layers:
            load(caches[2 * layer + 2], kv.at[2 * layer + 2], HEADS)
            load(caches[2 * layer + 3], kv.at[2 * layer + 3], HEADS)
        q64 = jnp.concatenate([pair_rows(q_all[layer, s % 2, s // 2].astype(jnp.float32)) for s in range(groups)], axis=0).astype(jnp.bfloat16)
        scores = jnp.zeros((ROWS, seq_dev * heads), jnp.float32)
        for b in range(batch):
            s = lax.dot_general(q64, kv[2 * layer, b], (((1,), (1,)), ((), ())), preferred_element_type=jnp.float32)
            s = jnp.where(hits[b], s, 0.0)
            for d in range(groups):
                scores = scores + s[d * ROWS:(d + 1) * ROWS]
        valid = paired
        if layer == 0:
            valid = valid & (me * seq_dev + wide_col // heads >= seq + 1 - WINDOW)
        scores = jnp.where(valid, scores * scale, NEG)
        m_loc = fold(scores, jnp.maximum)
        m_loc = jnp.where(own, jnp.maximum(m_loc, s_new), m_loc)
        ex = jnp.where(valid, jnp.exp(scores - jnp.tile(m_loc, (1, col_tiles))), 0.0)
        l_loc = fold(ex, jnp.add)
        l_loc = jnp.where(own, l_loc + jnp.exp(s_new - m_loc), l_loc)
        mine = lane // heads == row
        st_all[layer, me] = jnp.concatenate(
            [jnp.sum(jnp.where(mine, t, 0.0), axis=0, keepdims=True) for t in (m_loc, l_loc)], axis=0)
        got = start_round("all", [(st_all.at[layer, me], st_all.at[layer, me], (me + k) % groups) for k in range(1, groups)],
                          st_all.at[layer, pl.ds(0, groups - 1)])
        bulk(ROUND_UNITS[rnd + 1])
        got.wait_recv()
        def unpack(s, n):
            return fold(jnp.where(mine, jnp.broadcast_to(st_all[layer, s, n:n + 1, :], (ROWS, LANES)), 0.0), jnp.add)

        ms = [unpack(s, 0) for s in range(groups)]
        ls = [unpack(s, 1) for s in range(groups)]
        m_all = functools.reduce(jnp.maximum, ms)
        l_all = functools.reduce(jnp.add, [l * jnp.exp(m - m_all) for m, l in zip(ms, ls)])
        l_all = jnp.where(row < 2 * batch, jnp.maximum(l_all, 1e-30), 1.0)
        prob = jnp.where(valid, jnp.exp(scores - jnp.tile(m_all, (1, col_tiles))) / jnp.tile(l_all, (1, col_tiles)), 0.0)
        p_new = jnp.where(own & (lane < heads), jnp.exp(jnp.minimum(s_new - m_all, 0.0)) / l_all, 0.0)
        p_new = jnp.sum(p_new, axis=-1, keepdims=True).astype(jnp.bfloat16).astype(jnp.float32)
        prob64 = jnp.concatenate([prob] * groups, axis=0)
        weighted = jnp.zeros((groups * ROWS, head_dim), jnp.float32)
        for b in range(batch):
            weighted = weighted + jnp.dot(jnp.where(hits[b], prob64, 0.0).astype(jnp.bfloat16), kv[2 * layer + 1, b],
                                          preferred_element_type=jnp.float32)
        for d in range(groups):
            for b in range(batch):
                o_part[layer, d % 2, d // 2, b] = weighted[d * ROWS + 2 * b:d * ROWS + 2 * b + 2]
        o = scatter(o_part.at[layer], o_pair.at[layer], o_sum.at[layer], o_cross.at[layer], ROUND_UNITS[rnd + 2])
        o = pair_rows(o) + p_new * v_new
        o = o.astype(jnp.bfloat16).astype(jnp.float32)
        o = jnp.concatenate([jnp.where(even, o, 0.0), jnp.where(even, 0.0, o)], axis=-1).astype(jnp.bfloat16)
        wo_copy.wait()
        piece = width // groups
        for d in range(groups):
            y = jnp.dot(o, wo_buf[:, d * piece:(d + 1) * piece], preferred_element_type=jnp.float32)
            y = merge(y)
            for b in range(batch):
                part[2 * layer, d % 2, d // 2, b] = y[b:b + 1]
        if layer + 1 < layers:
            wo_copy = load(wo.at[layer + 1], wo_buf, OUT)
        hidden = h_ref[...] + rms_norm(all_reduce(rnd + 3, 2 * layer), ng[layer, 1:2, :])
        h_ref[...] = hidden
        lhs[...] = rms_norm(hidden, ng[layer, 2:3, :]).astype(jnp.bfloat16)
        stream(base + 3, 2 * ff_items)
        for n in range(ff_items):
            lhs[:, n * CHUNK:(n + 1) * CHUNK] = (
                jax.nn.gelu(acc[2 * n], approximate=True) * acc[2 * n + 1]).astype(jnp.bfloat16)
        stream(base + 3 + 2 * ff_items, wd_items)
        full = jnp.concatenate([acc[n] for n in range(wd_items)], axis=-1)
        for d in range(groups):
            for b in range(batch):
                part[2 * layer + 1, d % 2, d // 2, b] = full[b:b + 1, d * piece:(d + 1) * piece]
        hidden = h_ref[...] + rms_norm(all_reduce(rnd + 5, 2 * layer + 1), ng[layer, 3:4, :])
        h_ref[...] = hidden.astype(jnp.bfloat16).astype(jnp.float32)

    bulk(len(queue))
    for b in range(batch):
        h_out[b:b + 1, :] = h_ref[b:b + 1, :].astype(jnp.bfloat16)
    zeros = jnp.zeros((NEW_SLOTS - 1, 2, 2, LANES), jnp.bfloat16)
    for c in (2, 3):
        for b in range(batch):
            cache_out[c][b, seq + 1:] = zeros

    def store_new(c):
        for b in range(batch):
            for ct in range(2):
                cache_out[c][b, (seq % WINDOW, seq)[c // 2], ct] = new_rows[c // 2][c % 2][
                    2 * b:2 * b + 2, ct * LANES:(ct + 1) * LANES].astype(jnp.bfloat16)

    store_new(2)
    store_new(3)
    for c in pending:
        c.wait_send()
    own_rows = cache_out[0].at[0:batch, pl.ds(0, 4 * seq_dev)]
    pltpu.make_async_copy(own_rows, own_rows, local_sem.at[SELF]).wait()
    size_of = kv.at[:, :, pl.ds(0, (seq - seq_dev) * 2)]
    whole = pltpu.make_async_remote_copy(size_of, size_of, bulk_sem.at[0], bulk_sem.at[1],
                                         device_id={"tp": sibling}, device_id_type=MESH)
    whole.wait_recv()
    whole.wait_send()
    store_new(0)
    store_new(1)


def flush_kernel(*refs):
    n = (len(refs) - 1) // 2
    copies = [pltpu.make_async_copy(refs[i], refs[n + i], refs[-1].at[i]) for i in range(n)]
    for c in copies:
        c.start()
    for c in copies:
        c.wait()


def solution(mesh):
    groups = mesh.shape["tp"]
    cache_in = P("dp", "tp", None, None)
    cache_out = P("dp", None, "tp", None)
    token_spec = P("dp", None)
    col_split = P(None, None, "tp")
    row_split = P(None, "tp", None)
    replicated = P()

    def per_device(k_local, v_local, k_global, v_global, x_token, w_q, w_k, w_v, w_o, w_gate, w_up, w_down, norm_gain, qk_gain):
        batch, seq_dev, heads, head_dim = k_local.shape
        layers, width, _ = w_q.shape
        ff_dev = w_gate.shape[2]
        seq = seq_dev * groups
        tiles, pairs, cols = heads // 8, 4, head_dim // LANES
        caches = (k_local, v_local, k_global, v_global)
        views = [c.reshape(batch, seq_dev, tiles, pairs, 2, cols, LANES).transpose(0, 1, 2, 5, 3, 4, 6) for c in caches]
        flat = [c.reshape(batch, seq_dev * heads, head_dim) for c in caches]
        inv_freq = [b ** (-2.0 * np.arange(head_dim // 2) / head_dim) for b in ROPE_BASES]
        angles = [seq / s * f for s, f in zip(POS_SCALES, inv_freq)]
        rope = jnp.asarray(np.stack([np.stack([np.cos(a), np.sin(a)]) for a in angles]), jnp.float32)
        any_spec = pl.BlockSpec(memory_space=pl.ANY)
        vmem_spec = pl.BlockSpec(memory_space=pltpu.VMEM)
        cfg = (groups, layers, batch, seq_dev, heads, head_dim, width, ff_dev)
        slots = (WINDOW, WINDOW, seq + NEW_SLOTS, seq + NEW_SLOTS)
        piece = width // groups
        chips = groups // 2
        res = pl.pallas_call(
            functools.partial(kernel, cfg),
            in_specs=[any_spec] * 19,
            out_specs=[vmem_spec] * 5,
            out_shape=[pltpu.VMEM((batch, s, 2, 2, LANES), jnp.bfloat16) for s in slots]
            + [pltpu.VMEM((batch, width), jnp.bfloat16)],
            scratch_shapes=[
                pltpu.VMEM((RING, width, CHUNK), jnp.bfloat16),
                pltpu.VMEM((w_o.shape[1], width), jnp.bfloat16),
                pltpu.VMEM((4, batch, seq_dev * heads, head_dim), jnp.bfloat16),
                pltpu.VMEM(x_token.shape, jnp.bfloat16),
                pltpu.VMEM(norm_gain.shape, jnp.float32),
                pltpu.VMEM(qk_gain.shape, jnp.float32),
                pltpu.VMEM(rope.shape, jnp.float32),
                pltpu.VMEM((ROWS, width), jnp.float32),
                pltpu.VMEM((ROWS, width), jnp.bfloat16),
                pltpu.VMEM((2 * ff_dev // CHUNK, ROWS, CHUNK), jnp.float32),
                pltpu.VMEM((layers, 2, chips, batch, 2, head_dim), jnp.bfloat16),
                pltpu.VMEM((layers, groups, 2, LANES), jnp.float32),
                pltpu.VMEM((layers, 2, chips, batch, 2, head_dim), jnp.float32),
                *[pltpu.VMEM((layers, chips, batch, 2, head_dim), jnp.float32)] * 3,
                pltpu.VMEM((2 * layers, 2, chips, batch, 1, piece), jnp.float32),
                *[pltpu.VMEM((2 * layers, chips, batch, 1, piece), jnp.float32)] * 3,
                pltpu.VMEM((2 * layers, 2, chips, batch, 1, piece), jnp.float32),
                pltpu.SemaphoreType.DMA((RING,)),
                pltpu.SemaphoreType.DMA((7,)),
                pltpu.SemaphoreType.DMA((2,)),
                pltpu.SemaphoreType.DMA((2,)),
                pltpu.SemaphoreType.DMA((5,)),
            ],
            compiler_params=pltpu.CompilerParams(
                collective_id=0, has_side_effects=True, vmem_limit_bytes=44 * 1024 * 1024),
        )(*views, *flat, x_token, w_q, w_k, w_v, w_o, w_gate, w_up, w_down, norm_gain, qk_gain, rope)
        held = [pltpu.with_memory_space_constraint(y, pltpu.VMEM) for y in res]
        res = pl.pallas_call(
            flush_kernel,
            in_specs=[vmem_spec] * 5,
            out_specs=[any_spec] * 5,
            out_shape=[jax.ShapeDtypeStruct(y.shape, y.dtype) for y in res],
            scratch_shapes=[pltpu.SemaphoreType.DMA((5,))],
            compiler_params=pltpu.CompilerParams(has_side_effects=True, vmem_limit_bytes=1024 * 1024),
        )(*held)
        outs = [y.transpose(0, 1, 3, 2, 4).reshape(batch, y.shape[1], 2, head_dim) for y in res[:4]]
        return (res[4], *outs)

    return jax.shard_map(per_device, mesh=mesh, in_specs=(cache_in, cache_in, cache_in, cache_in, token_spec, col_split, col_split, col_split, row_split, col_split, col_split, row_split, replicated, replicated), out_specs=(token_spec, cache_out, cache_out, cache_out, cache_out), check_vma=False)
```

```python
import functools

import jax
import jax.numpy as jnp
import numpy as np
from jax import lax
from jax.experimental import pallas as pl
from jax.experimental.pallas import tpu as pltpu
from jax.sharding import PartitionSpec as P

WINDOW = 1024
NEW_SLOTS = 128
NORM_EPS = 1e-6
ROPE_BASES = (10000.0, 1000000.0)
POS_SCALES = (1.0, 8.0)
NEG = -3.0e38
MESH = pl.DeviceIdType.MESH
LANES = 128
ROWS = 8
RING = 8
CHUNK = 512
SPLITS = 4
FIRST_UNITS = 6
ROUND_UNITS = (2, 3, 2, 2, 6, 2, 2, 2, 3, 2, 2, 6, 2, 2)
ROUNDS = 7


def rms_norm(values, gain_vec):
    mean_sq = jnp.mean(values * values, axis=-1, keepdims=True)
    return values * lax.rsqrt(mean_sq + NORM_EPS) * (1.0 + gain_vec)


def kernel(cfg, *refs):
    groups, layers, batch, seq_dev, heads, head_dim, width, ff_dev = cfg
    n_in, n_out = 2 * len(range(4)) + 11, 5
    ins, outs, scr = refs[:n_in], refs[n_in:n_in + n_out], refs[n_in + n_out:]
    views, caches = ins[:4], ins[4:8]
    x_hbm, wq, wk, wv, wo, wg, wu, wd, ng_hbm, qk_hbm, rope_hbm = ins[8:]
    cache_out, h_out = outs[:4], outs[4]
    (ring, wo_buf, kv, x_vm, ng, qkg, rope, h_ref, lhs, acc, q_all, st_all, o_part, o_pair, o_sum, o_cross,
     part, rs_pair, rs_sum, rs_cross, ag_all,
     ring_sem, local_sem, bulk_sem, r_send, r_recv) = scr
    me = lax.axis_index("tp")
    per_tile = heads // 2
    pairs = per_tile // 2
    seq = seq_dev * groups
    half_dim = head_dim // 2
    ff_items = ff_dev // CHUNK
    wd_items = width // CHUNK
    per_layer = 3 + 2 * ff_items + wd_items
    items = layers * per_layer

    def issue(item):
        layer = item // per_layer
        r = item % per_layer
        slot = item % RING
        dst = ring.at[slot]
        sem = ring_sem.at[slot]
        for pos, ref in enumerate((wq, wk, wv)):
            @pl.when(r == pos)
            def _(ref=ref):
                pltpu.make_async_copy(ref.at[layer], dst, sem).start()
        for par, ref in enumerate((wg, wu)):
            @pl.when((r >= 3) & (r < 3 + 2 * ff_items) & ((r - 3) % 2 == par))
            def _(ref=ref):
                col = pl.multiple_of(jnp.clip((r - 3) // 2, 0, ff_items - 1) * CHUNK, CHUNK)
                pltpu.make_async_copy(ref.at[layer, :, pl.ds(col, CHUNK)], dst, sem).start()

        @pl.when(r >= 3 + 2 * ff_items)
        def _():
            col = pl.multiple_of(jnp.clip(r - 3 - 2 * ff_items, 0, wd_items - 1) * CHUNK, CHUNK)
            pltpu.make_async_copy(wd.at[layer, :, pl.ds(col, CHUNK)], dst, sem).start()

    def stream(first, count):
        def step(t, carry):
            item = first + t
            slot = item % RING
            pltpu.make_async_copy(wq.at[0], ring.at[slot], ring_sem.at[slot]).wait()
            acc[t] = jnp.dot(lhs[...], ring[slot], preferred_element_type=jnp.float32)

            @pl.when(item + RING < items)
            def _():
                issue(item + RING)
            return carry
        lax.fori_loop(0, count, step, 0)

    barrier = pltpu.get_barrier_semaphore()
    for k in range(1, groups):
        pl.semaphore_signal(barrier, inc=1, device_id={"tp": (me + k) % groups}, device_id_type=MESH)
    pl.semaphore_wait(barrier, groups - 1)

    span = seq_dev // SPLITS
    units = [(c, b, f) for c in range(4) for b in range(batch) for f in range(SPLITS)]
    chips = groups // 2
    order = [(0, 1)] + [(dx, dc) for dc in range(2) for dx in (1, chips - 1, *range(2, chips - 1))]
    chip, core = me // 2, me % 2

    def peer(dx, dc):
        return ((chip + dx) % chips) * 2 + (core + dc) % 2

    def view_of(c, owner, b, start, size):
        return views[c].at[b, pl.ds(start, size), owner // pairs, :, owner % pairs]

    queue = list(units)

    def bulk(count):
        for _ in range(min(count, len(queue))):
            c, b, f = queue.pop(0)
            for k, (dx, dc) in enumerate(order):
                dst = peer(dx, dc)
                pltpu.make_async_remote_copy(
                    view_of(c, dst, b, f * span, span),
                    cache_out[c].at[b, pl.ds(me * seq_dev + f * span, span)],
                    bulk_sem.at[0], bulk_sem.at[1],
                    device_id={"tp": dst}, device_id_type=MESH).start()

    bulk(FIRST_UNITS)
    def load(src, dst, which):
        c = pltpu.make_async_copy(src, dst, local_sem.at[which])
        c.start()
        return c

    SMALL, OUT, HEADS, SELF = range(4)
    small = ((x_hbm, x_vm), (ng_hbm, ng), (qk_hbm, qkg), (rope_hbm, rope))
    small_copies = [load(*small[0], SMALL)] + [load(*small[n], 3 + n) for n in (1, 2, 3)]
    for n in range(3):
        pltpu.make_async_copy((wq, wk, wv)[n].at[0], ring.at[n], ring_sem.at[n]).start()
    load(caches[0], kv.at[0], HEADS)
    load(caches[1], kv.at[1], HEADS)
    wo_copy = load(wo.at[0], wo_buf, OUT)
    for n in range(3, RING):
        issue(jnp.int32(n))
    for c in range(4):
        for b in range(batch):
            load(view_of(c, me, b, 0, seq_dev), cache_out[c].at[b, pl.ds(me * seq_dev, seq_dev)], SELF)

    sibling = chip * 2 + 1 - core
    turns = {"pair": 0, "cross": 0}
    pending = []

    def start_round(kind, copies, size_of):
        if len(pending) == 2:
            pending.pop(0).wait_send()
        turn = turns[kind]
        turns[kind] += 1
        s_sem = r_send.at[sum(turns.values()) % 2]
        r_sem = r_recv.at[{"pair": 0, "cross": 2}[kind] + turn % 2]
        for src, dst, device in copies:
            pltpu.make_async_remote_copy(src, dst, s_sem, r_sem, device_id={"tp": device}, device_id_type=MESH).start()
        pending.append(pltpu.make_async_remote_copy(size_of, size_of, s_sem, r_sem,
                                                    device_id={"tp": sibling}, device_id_type=MESH))
        return pending[-1]

    others = [(chip + dx) % chips for dx in (1, chips - 1, *range(2, chips - 1))]

    def gather_cross(ref, units):
        got = start_round("cross", [(ref.at[core, chip], ref.at[core, chip], t * 2 + core) for t in others],
                          ref.at[core, pl.ds(0, chips - 1)])
        bulk(units)
        got.wait_recv()

    def gather_pair(ref):
        start_round("pair", [(ref.at[core], ref.at[core], sibling)], ref.at[core]).wait_recv()

    def scatter(mine, pair, summed, cross, units):
        start_round("pair", [(mine.at[1 - core], pair, sibling)], pair).wait_recv()
        for t in range(chips):
            summed[t] = mine[core, t] + pair[t]
        got = start_round("cross", [(summed.at[t], cross.at[chip], t * 2 + core) for t in others],
                          cross.at[pl.ds(0, chips - 1)])
        bulk(units)
        cross[chip] = summed[chip]
        got.wait_recv()
        total = cross[0]
        for t in range(1, chips):
            total = total + cross[t]
        return total

    row = lax.broadcasted_iota(jnp.int32, (ROWS, LANES), 0)
    lane = lax.broadcasted_iota(jnp.int32, (ROWS, LANES), 1)
    even = lax.broadcasted_iota(jnp.int32, (ROWS, 1), 0) % 2 == 0
    lane_head = lane % heads
    own = (lane_head == 2 * me + row % 2) & (row < 2 * batch)
    col_tiles = seq_dev * heads // LANES
    row64 = lax.broadcasted_iota(jnp.int32, (groups * ROWS, LANES), 0)
    lane64 = lax.broadcasted_iota(jnp.int32, (groups * ROWS, LANES), 1)
    head_hit = (lane64 % heads) == 2 * (row64 // ROWS) + row64 % 2
    hits = [jnp.tile(head_hit & ((row64 % ROWS) // 2 == b), (1, col_tiles)) for b in range(batch)]
    wide_row = lax.broadcasted_iota(jnp.int32, (ROWS, seq_dev * heads), 0)
    wide_col = lax.broadcasted_iota(jnp.int32, (ROWS, seq_dev * heads), 1)
    paired = (wide_col % 2 == wide_row % 2) & (wide_row < 2 * batch)

    def fold(x, op):
        out = x[:, :LANES]
        for n in range(1, x.shape[1] // LANES):
            out = op(out, x[:, n * LANES:(n + 1) * LANES])
        shift = heads
        while shift < LANES:
            out = op(out, pltpu.roll(out, shift, 1))
            shift *= 2
        return out

    def rope_rotate(x, layer):
        cos, sin = rope[layer, 0:1, :], rope[layer, 1:2, :]
        a, b = x[:, :half_dim], x[:, half_dim:]
        return jnp.concatenate([a * cos - b * sin, b * cos + a * sin], axis=-1)

    row1 = lax.broadcasted_iota(jnp.int32, (ROWS, 1), 0)

    def pick(y):
        y = jnp.where(row1 == 0, y, jnp.where(row1 < 3, pltpu.roll(y, 1, 0), jnp.where(
            row1 < 5, pltpu.roll(y, 2, 0), pltpu.roll(y, 3, 0))))
        return jnp.where(even, y[:, :head_dim], y[:, head_dim:])

    def pair_rows(y):
        return jnp.concatenate([*(y[b] for b in range(batch)), jnp.zeros((ROWS - 2 * batch, head_dim), jnp.float32)], axis=0)

    def merge(y):
        y = y + pltpu.roll(y, ROWS - 1, 0)
        return jnp.where(row1 == 0, y, jnp.where(row1 == 1, pltpu.roll(y, ROWS - 1, 0), jnp.where(
            row1 == 2, pltpu.roll(y, ROWS - 2, 0), 0.0)))

    def all_reduce(rnd, slot):
        ag_all[slot, core, chip] = scatter(part.at[slot], rs_pair.at[slot], rs_sum.at[slot], rs_cross.at[slot],
                                           ROUND_UNITS[rnd])
        gather_cross(ag_all.at[slot], ROUND_UNITS[rnd + 1])
        gather_pair(ag_all.at[slot])
        whole = [jnp.concatenate([ag_all[slot, s % 2, s // 2, b] for s in range(groups)], axis=-1) for b in range(batch)]
        return jnp.concatenate([*whole, jnp.zeros((ROWS - batch, width), jnp.float32)], axis=0)

    for c in small_copies:
        c.wait()
    h_ref[...] = jnp.concatenate(
        [x_vm[...].astype(jnp.float32), jnp.zeros((ROWS - batch, width), jnp.float32)], axis=0)

    new_rows = []
    for layer in range(layers):
        rnd = layer * ROUNDS
        base = layer * per_layer
        lhs[...] = rms_norm(h_ref[...], ng[layer, 0:1, :]).astype(jnp.bfloat16)
        stream(base, 3)
        q = rope_rotate(rms_norm(pick(acc[0]), qkg[layer, 0:1, :]), layer).astype(jnp.bfloat16).astype(jnp.float32)
        for b in range(batch):
            q_all[layer, core, chip, b] = q[2 * b:2 * b + 2].astype(jnp.bfloat16)
        gather_cross(q_all.at[layer], ROUND_UNITS[rnd])
        gather_pair(q_all.at[layer])
        k_new = rope_rotate(rms_norm(pick(acc[1]), qkg[layer, 1:2, :]), layer).astype(jnp.bfloat16).astype(jnp.float32)
        v_new = pick(acc[2]).astype(jnp.bfloat16).astype(jnp.float32)
        new_rows.append((k_new, v_new))
        scale = head_dim ** -0.5
        s_new = jnp.sum(q * k_new, axis=-1, keepdims=True) * scale
        both = kv.at[2 * layer:2 * layer + 2]
        pltpu.make_async_copy(both, both, local_sem.at[HEADS]).wait()
        if layer + 1 < layers:
            load(caches[2 * layer + 2], kv.at[2 * layer + 2], HEADS)
            load(caches[2 * layer + 3], kv.at[2 * layer + 3], HEADS)
        q64 = jnp.concatenate([pair_rows(q_all[layer, s % 2, s // 2].astype(jnp.float32)) for s in range(groups)], axis=0).astype(jnp.bfloat16)
        scores = jnp.zeros((ROWS, seq_dev * heads), jnp.float32)
        for b in range(batch):
            s = lax.dot_general(q64, kv[2 * layer, b], (((1,), (1,)), ((), ())), preferred_element_type=jnp.float32)
            s = jnp.where(hits[b], s, 0.0)
            for d in range(groups):
                scores = scores + s[d * ROWS:(d + 1) * ROWS]
        valid = paired
        if layer == 0:
            valid = valid & (me * seq_dev + wide_col // heads >= seq + 1 - WINDOW)
        scores = jnp.where(valid, scores * scale, NEG)
        m_loc = fold(scores, jnp.maximum)
        m_loc = jnp.where(own, jnp.maximum(m_loc, s_new), m_loc)
        ex = jnp.where(valid, jnp.exp(scores - jnp.tile(m_loc, (1, col_tiles))), 0.0)
        l_loc = fold(ex, jnp.add)
        l_loc = jnp.where(own, l_loc + jnp.exp(s_new - m_loc), l_loc)
        mine = lane // heads == row
        st_all[layer, core, chip] = jnp.concatenate(
            [jnp.sum(jnp.where(mine, t, 0.0), axis=0, keepdims=True) for t in (m_loc, l_loc)], axis=0)
        gather_cross(st_all.at[layer], ROUND_UNITS[rnd + 1])
        gather_pair(st_all.at[layer])

        def unpack(s, n):
            return fold(jnp.where(mine, jnp.broadcast_to(st_all[layer, s % 2, s // 2, n:n + 1, :], (ROWS, LANES)), 0.0), jnp.add)

        ms = [unpack(s, 0) for s in range(groups)]
        ls = [unpack(s, 1) for s in range(groups)]
        m_all = functools.reduce(jnp.maximum, ms)
        l_all = functools.reduce(jnp.add, [l * jnp.exp(m - m_all) for m, l in zip(ms, ls)])
        l_all = jnp.where(row < 2 * batch, jnp.maximum(l_all, 1e-30), 1.0)
        prob = jnp.where(valid, jnp.exp(scores - jnp.tile(m_all, (1, col_tiles))) / jnp.tile(l_all, (1, col_tiles)), 0.0)
        p_new = jnp.where(own & (lane < heads), jnp.exp(jnp.minimum(s_new - m_all, 0.0)) / l_all, 0.0)
        p_new = jnp.sum(p_new, axis=-1, keepdims=True).astype(jnp.bfloat16).astype(jnp.float32)
        prob64 = jnp.concatenate([prob] * groups, axis=0)
        weighted = jnp.zeros((groups * ROWS, head_dim), jnp.float32)
        for b in range(batch):
            weighted = weighted + jnp.dot(jnp.where(hits[b], prob64, 0.0).astype(jnp.bfloat16), kv[2 * layer + 1, b],
                                          preferred_element_type=jnp.float32)
        for d in range(groups):
            for b in range(batch):
                o_part[layer, d % 2, d // 2, b] = weighted[d * ROWS + 2 * b:d * ROWS + 2 * b + 2]
        o = scatter(o_part.at[layer], o_pair.at[layer], o_sum.at[layer], o_cross.at[layer], ROUND_UNITS[rnd + 2])
        o = pair_rows(o) + p_new * v_new
        o = o.astype(jnp.bfloat16).astype(jnp.float32)
        o = jnp.concatenate([jnp.where(even, o, 0.0), jnp.where(even, 0.0, o)], axis=-1).astype(jnp.bfloat16)
        wo_copy.wait()
        piece = width // groups
        for d in range(groups):
            y = jnp.dot(o, wo_buf[:, d * piece:(d + 1) * piece], preferred_element_type=jnp.float32)
            y = merge(y)
            for b in range(batch):
                part[2 * layer, d % 2, d // 2, b] = y[b:b + 1]
        if layer + 1 < layers:
            wo_copy = load(wo.at[layer + 1], wo_buf, OUT)
        hidden = h_ref[...] + rms_norm(all_reduce(rnd + 3, 2 * layer), ng[layer, 1:2, :])
        h_ref[...] = hidden
        lhs[...] = rms_norm(hidden, ng[layer, 2:3, :]).astype(jnp.bfloat16)
        stream(base + 3, 2 * ff_items)
        for n in range(ff_items):
            lhs[:, n * CHUNK:(n + 1) * CHUNK] = (
                jax.nn.gelu(acc[2 * n], approximate=True) * acc[2 * n + 1]).astype(jnp.bfloat16)
        stream(base + 3 + 2 * ff_items, wd_items)
        full = jnp.concatenate([acc[n] for n in range(wd_items)], axis=-1)
        for d in range(groups):
            for b in range(batch):
                part[2 * layer + 1, d % 2, d // 2, b] = full[b:b + 1, d * piece:(d + 1) * piece]
        hidden = h_ref[...] + rms_norm(all_reduce(rnd + 5, 2 * layer + 1), ng[layer, 3:4, :])
        h_ref[...] = hidden.astype(jnp.bfloat16).astype(jnp.float32)

    bulk(len(queue))
    for b in range(batch):
        h_out[b:b + 1, :] = h_ref[b:b + 1, :].astype(jnp.bfloat16)
    zeros = jnp.zeros((NEW_SLOTS - 1, 2, 2, LANES), jnp.bfloat16)
    for c in (2, 3):
        for b in range(batch):
            cache_out[c][b, seq + 1:] = zeros

    def store_new(c):
        for b in range(batch):
            for ct in range(2):
                cache_out[c][b, (seq % WINDOW, seq)[c // 2], ct] = new_rows[c // 2][c % 2][
                    2 * b:2 * b + 2, ct * LANES:(ct + 1) * LANES].astype(jnp.bfloat16)

    store_new(2)
    store_new(3)
    for c in pending:
        c.wait_send()
    own_rows = cache_out[0].at[0:batch, pl.ds(0, 4 * seq_dev)]
    pltpu.make_async_copy(own_rows, own_rows, local_sem.at[SELF]).wait()
    size_of = kv.at[:, :, pl.ds(0, (seq - seq_dev) * 2)]
    whole = pltpu.make_async_remote_copy(size_of, size_of, bulk_sem.at[0], bulk_sem.at[1],
                                         device_id={"tp": sibling}, device_id_type=MESH)
    whole.wait_recv()
    whole.wait_send()
    store_new(0)
    store_new(1)


def flush_kernel(*refs):
    n = (len(refs) - 1) // 2
    pairs = [(refs[i].at[b], refs[n + i].at[b]) for i in range(n - 1) for b in range(refs[i].shape[0])]
    pairs.append((refs[n - 1], refs[2 * n - 1]))
    copies = [pltpu.make_async_copy(src, dst, refs[-1].at[i]) for i, (src, dst) in enumerate(pairs)]
    for i, c in enumerate(copies):
        c.start(priority=i % 2)
    for c in copies:
        c.wait()


def solution(mesh):
    groups = mesh.shape["tp"]
    cache_in = P("dp", "tp", None, None)
    cache_out = P("dp", None, "tp", None)
    token_spec = P("dp", None)
    col_split = P(None, None, "tp")
    row_split = P(None, "tp", None)
    replicated = P()

    def per_device(k_local, v_local, k_global, v_global, x_token, w_q, w_k, w_v, w_o, w_gate, w_up, w_down, norm_gain, qk_gain):
        batch, seq_dev, heads, head_dim = k_local.shape
        layers, width, _ = w_q.shape
        ff_dev = w_gate.shape[2]
        seq = seq_dev * groups
        tiles, pairs, cols = heads // 8, 4, head_dim // LANES
        caches = (k_local, v_local, k_global, v_global)
        views = [c.reshape(batch, seq_dev, tiles, pairs, 2, cols, LANES).transpose(0, 1, 2, 5, 3, 4, 6) for c in caches]
        flat = [c.reshape(batch, seq_dev * heads, head_dim) for c in caches]
        inv_freq = [b ** (-2.0 * np.arange(head_dim // 2) / head_dim) for b in ROPE_BASES]
        angles = [seq / s * f for s, f in zip(POS_SCALES, inv_freq)]
        rope = jnp.asarray(np.stack([np.stack([np.cos(a), np.sin(a)]) for a in angles]), jnp.float32)
        any_spec = pl.BlockSpec(memory_space=pl.ANY)
        vmem_spec = pl.BlockSpec(memory_space=pltpu.VMEM)
        cfg = (groups, layers, batch, seq_dev, heads, head_dim, width, ff_dev)
        slots = (WINDOW, WINDOW, seq + NEW_SLOTS, seq + NEW_SLOTS)
        piece = width // groups
        chips = groups // 2
        res = pl.pallas_call(
            functools.partial(kernel, cfg),
            in_specs=[any_spec] * 19,
            out_specs=[vmem_spec] * 5,
            out_shape=[pltpu.VMEM((batch, s, 2, 2, LANES), jnp.bfloat16) for s in slots]
            + [pltpu.VMEM((batch, width), jnp.bfloat16)],
            scratch_shapes=[
                pltpu.VMEM((RING, width, CHUNK), jnp.bfloat16),
                pltpu.VMEM((w_o.shape[1], width), jnp.bfloat16),
                pltpu.VMEM((4, batch, seq_dev * heads, head_dim), jnp.bfloat16),
                pltpu.VMEM(x_token.shape, jnp.bfloat16),
                pltpu.VMEM(norm_gain.shape, jnp.float32),
                pltpu.VMEM(qk_gain.shape, jnp.float32),
                pltpu.VMEM(rope.shape, jnp.float32),
                pltpu.VMEM((ROWS, width), jnp.float32),
                pltpu.VMEM((ROWS, width), jnp.bfloat16),
                pltpu.VMEM((2 * ff_dev // CHUNK, ROWS, CHUNK), jnp.float32),
                pltpu.VMEM((layers, 2, chips, batch, 2, head_dim), jnp.bfloat16),
                pltpu.VMEM((layers, 2, chips, 2, LANES), jnp.float32),
                pltpu.VMEM((layers, 2, chips, batch, 2, head_dim), jnp.float32),
                *[pltpu.VMEM((layers, chips, batch, 2, head_dim), jnp.float32)] * 3,
                pltpu.VMEM((2 * layers, 2, chips, batch, 1, piece), jnp.float32),
                *[pltpu.VMEM((2 * layers, chips, batch, 1, piece), jnp.float32)] * 3,
                pltpu.VMEM((2 * layers, 2, chips, batch, 1, piece), jnp.float32),
                pltpu.SemaphoreType.DMA((RING,)),
                pltpu.SemaphoreType.DMA((7,)),
                pltpu.SemaphoreType.DMA((2,)),
                pltpu.SemaphoreType.DMA((2,)),
                pltpu.SemaphoreType.DMA((4,)),
            ],
            compiler_params=pltpu.CompilerParams(
                collective_id=0, has_side_effects=True, vmem_limit_bytes=44 * 1024 * 1024),
        )(*views, *flat, x_token, w_q, w_k, w_v, w_o, w_gate, w_up, w_down, norm_gain, qk_gain, rope)
        held = [pltpu.with_memory_space_constraint(y, pltpu.VMEM) for y in res]
        res = pl.pallas_call(
            flush_kernel,
            in_specs=[vmem_spec] * 5,
            out_specs=[any_spec] * 5,
            out_shape=[jax.ShapeDtypeStruct(y.shape, y.dtype) for y in res],
            scratch_shapes=[pltpu.SemaphoreType.DMA((4 * batch + 1,))],
            compiler_params=pltpu.CompilerParams(has_side_effects=True, vmem_limit_bytes=1024 * 1024),
        )(*held)
        outs = [y.transpose(0, 1, 3, 2, 4).reshape(batch, y.shape[1], 2, head_dim) for y in res[:4]]
        return (res[4], *outs)

    return jax.shard_map(per_device, mesh=mesh, in_specs=(cache_in, cache_in, cache_in, cache_in, token_spec, col_split, col_split, col_split, row_split, col_split, col_split, row_split, replicated, replicated), out_specs=(token_spec, cache_out, cache_out, cache_out, cache_out), check_vma=False)
```

```python
import functools

import jax
import jax.numpy as jnp
import numpy as np
from jax import lax
from jax.experimental import pallas as pl
from jax.experimental.pallas import tpu as pltpu
from jax.sharding import PartitionSpec as P

WINDOW = 1024
NEW_SLOTS = 128
NORM_EPS = 1e-6
ROPE_BASES = (10000.0, 1000000.0)
POS_SCALES = (1.0, 8.0)
NEG = -3.0e38
MESH = pl.DeviceIdType.MESH
LANES = 128
ROWS = 8
RING = 8
CHUNK = 512
SPLITS = 4
FIRST_UNITS = 5
ROUND_UNITS = (2, 3, 2, 2, 6, 2, 3, 2, 3, 2, 2, 6, 2, 2)
ROUNDS = 7


def rms_norm(values, gain_vec):
    mean_sq = jnp.mean(values * values, axis=-1, keepdims=True)
    return values * lax.rsqrt(mean_sq + NORM_EPS) * (1.0 + gain_vec)


def kernel(cfg, *refs):
    groups, layers, batch, seq_dev, heads, head_dim, width, ff_dev = cfg
    n_in, n_out = 2 * len(range(4)) + 11, 5
    ins, outs, scr = refs[:n_in], refs[n_in:n_in + n_out], refs[n_in + n_out:]
    views, caches = ins[:4], ins[4:8]
    x_hbm, wq, wk, wv, wo, wg, wu, wd, ng_hbm, qk_hbm, rope_hbm = ins[8:]
    cache_out, h_out = outs[:4], outs[4]
    (ring, wo_buf, kv, x_vm, ng, qkg, rope, h_ref, lhs, acc, q_all, st_all, o_part, o_pair, o_sum, o_cross,
     part, rs_pair, rs_sum, rs_cross, ag_all,
     ring_sem, local_sem, bulk_sem, r_send, r_recv) = scr
    me = lax.axis_index("tp")
    per_tile = heads // 2
    pairs = per_tile // 2
    seq = seq_dev * groups
    half_dim = head_dim // 2
    ff_items = ff_dev // CHUNK
    wd_items = width // CHUNK
    per_layer = 3 + 2 * ff_items + wd_items
    items = layers * per_layer

    def issue(item):
        layer = item // per_layer
        r = item % per_layer
        slot = item % RING
        dst = ring.at[slot]
        sem = ring_sem.at[slot]
        for pos, ref in enumerate((wq, wk, wv)):
            @pl.when(r == pos)
            def _(ref=ref):
                pltpu.make_async_copy(ref.at[layer], dst, sem).start()
        for par, ref in enumerate((wg, wu)):
            @pl.when((r >= 3) & (r < 3 + 2 * ff_items) & ((r - 3) % 2 == par))
            def _(ref=ref):
                col = pl.multiple_of(jnp.clip((r - 3) // 2, 0, ff_items - 1) * CHUNK, CHUNK)
                pltpu.make_async_copy(ref.at[layer, :, pl.ds(col, CHUNK)], dst, sem).start()

        @pl.when(r >= 3 + 2 * ff_items)
        def _():
            col = pl.multiple_of(jnp.clip(r - 3 - 2 * ff_items, 0, wd_items - 1) * CHUNK, CHUNK)
            pltpu.make_async_copy(wd.at[layer, :, pl.ds(col, CHUNK)], dst, sem).start()

    def stream(first, count):
        def step(t, carry):
            item = first + t
            slot = item % RING
            pltpu.make_async_copy(wq.at[0], ring.at[slot], ring_sem.at[slot]).wait()
            acc[t] = jnp.dot(lhs[...], ring[slot], preferred_element_type=jnp.float32)

            @pl.when(item + RING < items)
            def _():
                issue(item + RING)
            return carry
        lax.fori_loop(0, count, step, 0)

    barrier = pltpu.get_barrier_semaphore()
    for k in range(1, groups):
        pl.semaphore_signal(barrier, inc=1, device_id={"tp": (me + k) % groups}, device_id_type=MESH)
    pl.semaphore_wait(barrier, groups - 1)

    span = seq_dev // SPLITS
    units = [(c, b, f) for c in range(4) for b in range(batch) for f in range(SPLITS)]
    chips = groups // 2
    order = [(0, 1)] + [(dx, dc) for dc in range(2) for dx in (1, chips - 1, *range(2, chips - 1))]
    chip, core = me // 2, me % 2

    def peer(dx, dc):
        return ((chip + dx) % chips) * 2 + (core + dc) % 2

    def view_of(c, owner, b, start, size):
        return views[c].at[b, pl.ds(start, size), owner // pairs, :, owner % pairs]

    queue = list(units)

    def bulk(count):
        for _ in range(min(count, len(queue))):
            c, b, f = queue.pop(0)
            for k, (dx, dc) in enumerate(order):
                dst = peer(dx, dc)
                pltpu.make_async_remote_copy(
                    view_of(c, dst, b, f * span, span),
                    cache_out[c].at[b, pl.ds(me * seq_dev + f * span, span)],
                    bulk_sem.at[0], bulk_sem.at[1],
                    device_id={"tp": dst}, device_id_type=MESH).start()

    bulk(FIRST_UNITS)
    def load(src, dst, which):
        c = pltpu.make_async_copy(src, dst, local_sem.at[which])
        c.start()
        return c

    SMALL, OUT, HEADS, SELF = range(4)
    small = ((x_hbm, x_vm), (ng_hbm, ng), (qk_hbm, qkg), (rope_hbm, rope))
    small_copies = [load(*small[0], SMALL)] + [load(*small[n], 3 + n) for n in (1, 2, 3)]
    for n in range(3):
        pltpu.make_async_copy((wq, wk, wv)[n].at[0], ring.at[n], ring_sem.at[n]).start()
    load(caches[0], kv.at[0], HEADS)
    load(caches[1], kv.at[1], HEADS)
    wo_copy = load(wo.at[0], wo_buf, OUT)
    for n in range(3, RING):
        issue(jnp.int32(n))
    for c in range(4):
        for b in range(batch):
            load(view_of(c, me, b, 0, seq_dev), cache_out[c].at[b, pl.ds(me * seq_dev, seq_dev)], SELF)

    sibling = chip * 2 + 1 - core
    turns = {"pair": 0, "cross": 0}
    pending = []

    def start_round(kind, copies, size_of):
        if len(pending) == 2:
            pending.pop(0).wait_send()
        turn = turns[kind]
        turns[kind] += 1
        s_sem = r_send.at[sum(turns.values()) % 2]
        r_sem = r_recv.at[{"pair": 0, "cross": 2}[kind] + turn % 2]
        for src, dst, device in copies:
            pltpu.make_async_remote_copy(src, dst, s_sem, r_sem, device_id={"tp": device}, device_id_type=MESH).start()
        pending.append(pltpu.make_async_remote_copy(size_of, size_of, s_sem, r_sem,
                                                    device_id={"tp": sibling}, device_id_type=MESH))
        return pending[-1]

    others = [(chip + dx) % chips for dx in (1, chips - 1, *range(2, chips - 1))]

    def gather_cross(ref, units):
        got = start_round("cross", [(ref.at[core, chip], ref.at[core, chip], t * 2 + core) for t in others],
                          ref.at[core, pl.ds(0, chips - 1)])
        bulk(units)
        got.wait_recv()

    def gather_pair(ref):
        start_round("pair", [(ref.at[core], ref.at[core], sibling)], ref.at[core]).wait_recv()

    def scatter(mine, pair, summed, cross, units):
        start_round("pair", [(mine.at[1 - core], pair, sibling)], pair).wait_recv()
        for t in range(chips):
            summed[t] = mine[core, t] + pair[t]
        got = start_round("cross", [(summed.at[t], cross.at[chip], t * 2 + core) for t in others],
                          cross.at[pl.ds(0, chips - 1)])
        bulk(units)
        cross[chip] = summed[chip]
        got.wait_recv()
        total = cross[0]
        for t in range(1, chips):
            total = total + cross[t]
        return total

    row = lax.broadcasted_iota(jnp.int32, (ROWS, LANES), 0)
    lane = lax.broadcasted_iota(jnp.int32, (ROWS, LANES), 1)
    even = lax.broadcasted_iota(jnp.int32, (ROWS, 1), 0) % 2 == 0
    lane_head = lane % heads
    own = (lane_head == 2 * me + row % 2) & (row < 2 * batch)
    col_tiles = seq_dev * heads // LANES
    row64 = lax.broadcasted_iota(jnp.int32, (groups * ROWS, LANES), 0)
    lane64 = lax.broadcasted_iota(jnp.int32, (groups * ROWS, LANES), 1)
    head_hit = (lane64 % heads) == 2 * (row64 // ROWS) + row64 % 2
    hits = [jnp.tile(head_hit & ((row64 % ROWS) // 2 == b), (1, col_tiles)) for b in range(batch)]
    wide_row = lax.broadcasted_iota(jnp.int32, (ROWS, seq_dev * heads), 0)
    wide_col = lax.broadcasted_iota(jnp.int32, (ROWS, seq_dev * heads), 1)
    paired = (wide_col % 2 == wide_row % 2) & (wide_row < 2 * batch)

    def fold(x, op):
        out = x[:, :LANES]
        for n in range(1, x.shape[1] // LANES):
            out = op(out, x[:, n * LANES:(n + 1) * LANES])
        shift = heads
        while shift < LANES:
            out = op(out, pltpu.roll(out, shift, 1))
            shift *= 2
        return out

    def rope_rotate(x, layer):
        cos, sin = rope[layer, 0:1, :], rope[layer, 1:2, :]
        a, b = x[:, :half_dim], x[:, half_dim:]
        return jnp.concatenate([a * cos - b * sin, b * cos + a * sin], axis=-1)

    row1 = lax.broadcasted_iota(jnp.int32, (ROWS, 1), 0)

    def pick(y):
        y = jnp.where(row1 == 0, y, jnp.where(row1 < 3, pltpu.roll(y, 1, 0), jnp.where(
            row1 < 5, pltpu.roll(y, 2, 0), pltpu.roll(y, 3, 0))))
        return jnp.where(even, y[:, :head_dim], y[:, head_dim:])

    def pair_rows(y):
        return jnp.concatenate([*(y[b] for b in range(batch)), jnp.zeros((ROWS - 2 * batch, head_dim), jnp.float32)], axis=0)

    def merge(y):
        y = y + pltpu.roll(y, ROWS - 1, 0)
        return jnp.where(row1 == 0, y, jnp.where(row1 == 1, pltpu.roll(y, ROWS - 1, 0), jnp.where(
            row1 == 2, pltpu.roll(y, ROWS - 2, 0), 0.0)))

    def all_reduce(rnd, slot):
        ag_all[slot, core, chip] = scatter(part.at[slot], rs_pair.at[slot], rs_sum.at[slot], rs_cross.at[slot],
                                           ROUND_UNITS[rnd])
        gather_cross(ag_all.at[slot], ROUND_UNITS[rnd + 1])
        gather_pair(ag_all.at[slot])
        whole = [jnp.concatenate([ag_all[slot, s % 2, s // 2, b] for s in range(groups)], axis=-1) for b in range(batch)]
        return jnp.concatenate([*whole, jnp.zeros((ROWS - batch, width), jnp.float32)], axis=0)

    for c in small_copies:
        c.wait()
    h_ref[...] = jnp.concatenate(
        [x_vm[...].astype(jnp.float32), jnp.zeros((ROWS - batch, width), jnp.float32)], axis=0)

    new_rows = []
    for layer in range(layers):
        rnd = layer * ROUNDS
        base = layer * per_layer
        lhs[...] = rms_norm(h_ref[...], ng[layer, 0:1, :]).astype(jnp.bfloat16)
        stream(base, 3)
        q = rope_rotate(rms_norm(pick(acc[0]), qkg[layer, 0:1, :]), layer).astype(jnp.bfloat16).astype(jnp.float32)
        for b in range(batch):
            q_all[layer, core, chip, b] = q[2 * b:2 * b + 2].astype(jnp.bfloat16)
        gather_cross(q_all.at[layer], ROUND_UNITS[rnd])
        gather_pair(q_all.at[layer])
        k_new = rope_rotate(rms_norm(pick(acc[1]), qkg[layer, 1:2, :]), layer).astype(jnp.bfloat16).astype(jnp.float32)
        v_new = pick(acc[2]).astype(jnp.bfloat16).astype(jnp.float32)
        new_rows.append((k_new, v_new))
        scale = head_dim ** -0.5
        s_new = jnp.sum(q * k_new, axis=-1, keepdims=True) * scale
        both = kv.at[2 * layer:2 * layer + 2]
        pltpu.make_async_copy(both, both, local_sem.at[HEADS]).wait()
        if layer + 1 < layers:
            load(caches[2 * layer + 2], kv.at[2 * layer + 2], HEADS)
            load(caches[2 * layer + 3], kv.at[2 * layer + 3], HEADS)
        q64 = jnp.concatenate([pair_rows(q_all[layer, s % 2, s // 2].astype(jnp.float32)) for s in range(groups)], axis=0).astype(jnp.bfloat16)
        scores = jnp.zeros((ROWS, seq_dev * heads), jnp.float32)
        for b in range(batch):
            s = lax.dot_general(q64, kv[2 * layer, b], (((1,), (1,)), ((), ())), preferred_element_type=jnp.float32)
            s = jnp.where(hits[b], s, 0.0)
            for d in range(groups):
                scores = scores + s[d * ROWS:(d + 1) * ROWS]
        valid = paired
        if layer == 0:
            valid = valid & (me * seq_dev + wide_col // heads >= seq + 1 - WINDOW)
        scores = jnp.where(valid, scores * scale, NEG)
        m_loc = fold(scores, jnp.maximum)
        m_loc = jnp.where(own, jnp.maximum(m_loc, s_new), m_loc)
        ex = jnp.where(valid, jnp.exp(scores - jnp.tile(m_loc, (1, col_tiles))), 0.0)
        l_loc = fold(ex, jnp.add)
        l_loc = jnp.where(own, l_loc + jnp.exp(s_new - m_loc), l_loc)
        mine = lane // heads == row
        st_all[layer, core, chip] = jnp.concatenate(
            [jnp.sum(jnp.where(mine, t, 0.0), axis=0, keepdims=True) for t in (m_loc, l_loc)], axis=0)
        gather_cross(st_all.at[layer], ROUND_UNITS[rnd + 1])
        gather_pair(st_all.at[layer])

        def unpack(s, n):
            return fold(jnp.where(mine, jnp.broadcast_to(st_all[layer, s % 2, s // 2, n:n + 1, :], (ROWS, LANES)), 0.0), jnp.add)

        ms = [unpack(s, 0) for s in range(groups)]
        ls = [unpack(s, 1) for s in range(groups)]
        m_all = functools.reduce(jnp.maximum, ms)
        l_all = functools.reduce(jnp.add, [l * jnp.exp(m - m_all) for m, l in zip(ms, ls)])
        l_all = jnp.where(row < 2 * batch, jnp.maximum(l_all, 1e-30), 1.0)
        prob = jnp.where(valid, jnp.exp(scores - jnp.tile(m_all, (1, col_tiles))) / jnp.tile(l_all, (1, col_tiles)), 0.0)
        p_new = jnp.where(own & (lane < heads), jnp.exp(jnp.minimum(s_new - m_all, 0.0)) / l_all, 0.0)
        p_new = jnp.sum(p_new, axis=-1, keepdims=True).astype(jnp.bfloat16).astype(jnp.float32)
        prob64 = jnp.concatenate([prob] * groups, axis=0)
        weighted = jnp.zeros((groups * ROWS, head_dim), jnp.float32)
        for b in range(batch):
            weighted = weighted + jnp.dot(jnp.where(hits[b], prob64, 0.0).astype(jnp.bfloat16), kv[2 * layer + 1, b],
                                          preferred_element_type=jnp.float32)
        for d in range(groups):
            for b in range(batch):
                o_part[layer, d % 2, d // 2, b] = weighted[d * ROWS + 2 * b:d * ROWS + 2 * b + 2]
        o = scatter(o_part.at[layer], o_pair.at[layer], o_sum.at[layer], o_cross.at[layer], ROUND_UNITS[rnd + 2])
        o = pair_rows(o) + p_new * v_new
        o = o.astype(jnp.bfloat16).astype(jnp.float32)
        o = jnp.concatenate([jnp.where(even, o, 0.0), jnp.where(even, 0.0, o)], axis=-1).astype(jnp.bfloat16)
        wo_copy.wait()
        piece = width // groups
        for d in range(groups):
            y = jnp.dot(o, wo_buf[:, d * piece:(d + 1) * piece], preferred_element_type=jnp.float32)
            y = merge(y)
            for b in range(batch):
                part[2 * layer, d % 2, d // 2, b] = y[b:b + 1]
        if layer + 1 < layers:
            wo_copy = load(wo.at[layer + 1], wo_buf, OUT)
        hidden = h_ref[...] + rms_norm(all_reduce(rnd + 3, 2 * layer), ng[layer, 1:2, :])
        h_ref[...] = hidden
        lhs[...] = rms_norm(hidden, ng[layer, 2:3, :]).astype(jnp.bfloat16)
        stream(base + 3, 2 * ff_items)
        for n in range(ff_items):
            lhs[:, n * CHUNK:(n + 1) * CHUNK] = (
                jax.nn.gelu(acc[2 * n], approximate=True) * acc[2 * n + 1]).astype(jnp.bfloat16)
        stream(base + 3 + 2 * ff_items, wd_items)
        full = jnp.concatenate([acc[n] for n in range(wd_items)], axis=-1)
        for d in range(groups):
            for b in range(batch):
                part[2 * layer + 1, d % 2, d // 2, b] = full[b:b + 1, d * piece:(d + 1) * piece]
        hidden = h_ref[...] + rms_norm(all_reduce(rnd + 5, 2 * layer + 1), ng[layer, 3:4, :])
        h_ref[...] = hidden.astype(jnp.bfloat16).astype(jnp.float32)

    bulk(len(queue))
    for b in range(batch):
        h_out[b:b + 1, :] = h_ref[b:b + 1, :].astype(jnp.bfloat16)
    zeros = jnp.zeros((NEW_SLOTS - 1, 2, 2, LANES), jnp.bfloat16)
    for c in (2, 3):
        for b in range(batch):
            cache_out[c][b, seq + 1:] = zeros

    def store_new(c):
        for b in range(batch):
            for ct in range(2):
                cache_out[c][b, (seq % WINDOW, seq)[c // 2], ct] = new_rows[c // 2][c % 2][
                    2 * b:2 * b + 2, ct * LANES:(ct + 1) * LANES].astype(jnp.bfloat16)

    store_new(2)
    store_new(3)
    for c in pending:
        c.wait_send()
    own_rows = cache_out[0].at[0:batch, pl.ds(0, 4 * seq_dev)]
    pltpu.make_async_copy(own_rows, own_rows, local_sem.at[SELF]).wait()
    size_of = kv.at[:, :, pl.ds(0, (seq - seq_dev) * 2)]
    whole = pltpu.make_async_remote_copy(size_of, size_of, bulk_sem.at[0], bulk_sem.at[1],
                                         device_id={"tp": sibling}, device_id_type=MESH)
    whole.wait_recv()
    whole.wait_send()
    store_new(0)
    store_new(1)


def flush_kernel(*refs):
    n = (len(refs) - 1) // 2
    pairs = [(refs[i].at[b], refs[n + i].at[b]) for i in range(n - 1) for b in range(refs[i].shape[0])]
    pairs.append((refs[n - 1], refs[2 * n - 1]))
    copies = [pltpu.make_async_copy(src, dst, refs[-1].at[i]) for i, (src, dst) in enumerate(pairs)]
    for i, c in enumerate(copies):
        c.start(priority=i % 2)
    for c in copies:
        c.wait()


def solution(mesh):
    groups = mesh.shape["tp"]
    cache_in = P("dp", "tp", None, None)
    cache_out = P("dp", None, "tp", None)
    token_spec = P("dp", None)
    col_split = P(None, None, "tp")
    row_split = P(None, "tp", None)
    replicated = P()

    def per_device(k_local, v_local, k_global, v_global, x_token, w_q, w_k, w_v, w_o, w_gate, w_up, w_down, norm_gain, qk_gain):
        batch, seq_dev, heads, head_dim = k_local.shape
        layers, width, _ = w_q.shape
        ff_dev = w_gate.shape[2]
        seq = seq_dev * groups
        tiles, pairs, cols = heads // 8, 4, head_dim // LANES
        caches = (k_local, v_local, k_global, v_global)
        views = [c.reshape(batch, seq_dev, tiles, pairs, 2, cols, LANES).transpose(0, 1, 2, 5, 3, 4, 6) for c in caches]
        flat = [c.reshape(batch, seq_dev * heads, head_dim) for c in caches]
        inv_freq = [b ** (-2.0 * np.arange(head_dim // 2) / head_dim) for b in ROPE_BASES]
        angles = [seq / s * f for s, f in zip(POS_SCALES, inv_freq)]
        rope = jnp.asarray(np.stack([np.stack([np.cos(a), np.sin(a)]) for a in angles]), jnp.float32)
        any_spec = pl.BlockSpec(memory_space=pl.ANY)
        vmem_spec = pl.BlockSpec(memory_space=pltpu.VMEM)
        cfg = (groups, layers, batch, seq_dev, heads, head_dim, width, ff_dev)
        slots = (WINDOW, WINDOW, seq + NEW_SLOTS, seq + NEW_SLOTS)
        piece = width // groups
        chips = groups // 2
        res = pl.pallas_call(
            functools.partial(kernel, cfg),
            in_specs=[any_spec] * 19,
            out_specs=[vmem_spec] * 5,
            out_shape=[pltpu.VMEM((batch, s, 2, 2, LANES), jnp.bfloat16) for s in slots]
            + [pltpu.VMEM((batch, width), jnp.bfloat16)],
            scratch_shapes=[
                pltpu.VMEM((RING, width, CHUNK), jnp.bfloat16),
                pltpu.VMEM((w_o.shape[1], width), jnp.bfloat16),
                pltpu.VMEM((4, batch, seq_dev * heads, head_dim), jnp.bfloat16),
                pltpu.VMEM(x_token.shape, jnp.bfloat16),
                pltpu.VMEM(norm_gain.shape, jnp.float32),
                pltpu.VMEM(qk_gain.shape, jnp.float32),
                pltpu.VMEM(rope.shape, jnp.float32),
                pltpu.VMEM((ROWS, width), jnp.float32),
                pltpu.VMEM((ROWS, width), jnp.bfloat16),
                pltpu.VMEM((2 * ff_dev // CHUNK, ROWS, CHUNK), jnp.float32),
                pltpu.VMEM((layers, 2, chips, batch, 2, head_dim), jnp.bfloat16),
                pltpu.VMEM((layers, 2, chips, 2, LANES), jnp.float32),
                pltpu.VMEM((layers, 2, chips, batch, 2, head_dim), jnp.float32),
                *[pltpu.VMEM((layers, chips, batch, 2, head_dim), jnp.float32)] * 3,
                pltpu.VMEM((2 * layers, 2, chips, batch, 1, piece), jnp.float32),
                *[pltpu.VMEM((2 * layers, chips, batch, 1, piece), jnp.float32)] * 3,
                pltpu.VMEM((2 * layers, 2, chips, batch, 1, piece), jnp.float32),
                pltpu.SemaphoreType.DMA((RING,)),
                pltpu.SemaphoreType.DMA((7,)),
                pltpu.SemaphoreType.DMA((2,)),
                pltpu.SemaphoreType.DMA((2,)),
                pltpu.SemaphoreType.DMA((4,)),
            ],
            compiler_params=pltpu.CompilerParams(
                collective_id=0, has_side_effects=True, vmem_limit_bytes=44 * 1024 * 1024),
        )(*views, *flat, x_token, w_q, w_k, w_v, w_o, w_gate, w_up, w_down, norm_gain, qk_gain, rope)
        held = [pltpu.with_memory_space_constraint(y, pltpu.VMEM) for y in res]
        res = pl.pallas_call(
            flush_kernel,
            in_specs=[vmem_spec] * 5,
            out_specs=[any_spec] * 5,
            out_shape=[jax.ShapeDtypeStruct(y.shape, y.dtype) for y in res],
            scratch_shapes=[pltpu.SemaphoreType.DMA((4 * batch + 1,))],
            compiler_params=pltpu.CompilerParams(has_side_effects=True, vmem_limit_bytes=1024 * 1024),
        )(*held)
        outs = [y.transpose(0, 1, 3, 2, 4).reshape(batch, y.shape[1], 2, head_dim) for y in res[:4]]
        return (res[4], *outs)

    return jax.shard_map(per_device, mesh=mesh, in_specs=(cache_in, cache_in, cache_in, cache_in, token_spec, col_split, col_split, col_split, row_split, col_split, col_split, row_split, replicated, replicated), out_specs=(token_spec, cache_out, cache_out, cache_out, cache_out), check_vma=False)
```
